256 devices in a mesh: dev: 128 (over z, y, x), rep: 2 (over core).
Axes of the slice: x: 4, y: 4, z: 8, core: 2. Of those that a mesh axis runs over, the one named last changes fastest.
Arguments:
- tables: bfloat16 [512, 2048, 128], P('dev'), may hold values from -1.5 to 1.5
- bag_rows: int32 [256, 512, 32, 4], P(('rep', 'dev')), parts along dimension 0, may hold values from 0 to 2047
- bag_lengths: int32 [256, 512, 32], P(('rep', 'dev')), parts along dimension 0, may hold values from 1 to 4
- row_counts: int32 [256, 512], P(('rep', 'dev')), parts along dimension 0, may hold values from 1 to 32, as said below
- inverse: int32 [32768, 512], P(('rep', 'dev')), parts along dimension 0, may hold values from 0 to 31
- table_order: int32 [512], replicated, may hold values from 0 to 511, each once
- compress: bfloat16 [16, 512], replicated, may hold values from -0.25 to 0.25
- top_weight: bfloat16 [8192, 512], replicated, may hold values from -0.0625 to 0.0625
- top_bias: float32 [512], replicated, may hold values from -1.8 to 1.8
Outputs:
- ranked: bfloat16 [32768, 512], P(('rep', 'dev')), parts along dimension 0
The draws below stay inside these ranges and needn't reach their ends.
There are 2 independent parts, one for each index of `rep`. The reference program is written for one: setup_inputs(seed, part) draws one part's arguments, and reference() takes and returns one part's arrays. A program takes and returns all parts, laid end to end along the dimension named above; an argument that names none is the same for every part. Nothing has to cross between parts.
Inputs may be any that keep to these rules, and one draw needn't show every extreme that they name: `row_counts`: for every sample device and every aligned group of 4 consecutive slots the counts sum to at most 80; a count of 32 and a group sum of 80 occur in every draw.
All inputs are finite; a program needn't handle non-finite values.
Results may differ from the reference program's by a relative error of at most 0.0062.
Values may be sent and summed in bfloat16 or wider, within the bound.
No kernel may reach another device: no remote copies, remote signals or barrier semaphores. Data moves between devices by JAX's collectives and lax.ppermute only.
A program may use at most 128 MiB of HBM per device.

```python
import math
import jax
import jax.numpy as jnp
import numpy as np
from jax import lax

WIDTH = 128
VOCABULARY = 2048
TABLES_DEV = 4
TABLES = 512
BATCH_DEV = 128
BATCH = 16384
ROWS_MOST = 32
PACK_ROOM = 80
POOLING = 4
COMPRESSED = 16
TOP_UNITS = 512
N_DEV = 128


def draw_row_counts(key, part):
    first_key = jax.random.fold_in(key, 11)
    second_key = jax.random.fold_in(key, 12)
    third_key = jax.random.fold_in(key, 13)
    raw_counts = jax.random.randint(first_key, (N_DEV, N_DEV, TABLES_DEV), 1, ROWS_MOST + 1)
    group_total = jnp.sum(raw_counts, axis=2, keepdims=True)
    shrunk = 1 + (raw_counts - 1) * (PACK_ROOM - TABLES_DEV) // jnp.maximum(group_total - TABLES_DEV, 1)
    scaled = jnp.where(group_total > PACK_ROOM, shrunk, raw_counts)
    shift_value = jax.random.randint(second_key, (), 0, 5)
    device_range = jnp.arange(N_DEV, dtype=jnp.int32)[:, None]
    group_range = jnp.arange(N_DEV, dtype=jnp.int32)[None, :]
    forced = (device_range * 3 + group_range + shift_value) % 5 == 0
    leader = jax.random.randint(third_key, (N_DEV, N_DEV), 0, TABLES_DEV)
    remainder = PACK_ROOM - ROWS_MOST
    share_value = remainder // (TABLES_DEV - 1)
    last_value = remainder - (TABLES_DEV - 2) * share_value
    member = jnp.arange(TABLES_DEV, dtype=jnp.int32)[None, None, :]
    ranking = (member - leader[..., None]) % TABLES_DEV
    filled = jnp.where(ranking == 0, ROWS_MOST, jnp.where(ranking == TABLES_DEV - 1, last_value, share_value))
    result = jnp.where(forced[..., None], filled, scaled)
    return result.reshape(N_DEV, TABLES).astype(jnp.int32)


def with_ends(values, rng, smallest, largest):
    longest = values.shape.index(max(values.shape))
    spots = []
    for shift in (0, 1):
        where = [jax.random.randint(jax.random.fold_in(rng, axis), (), 0, length) for axis, length in enumerate(values.shape)]
        where[longest] = (where[longest] + shift) % values.shape[longest]
        spots.append(tuple(where))
    return values.at[spots[0]].set(smallest).at[spots[1]].set(largest)


def levels(own_key, dims, cuts, least, top_value):
    factor_of, own = 1.0, jax.random.fold_in(own_key, 6)
    for axis_at, blocks in cuts:
        heights = jnp.exp(jax.random.uniform(jax.random.fold_in(own, axis_at), (blocks,), jnp.float32, least / len(cuts), top_value / len(cuts)))
        factor_of = factor_of * jnp.repeat(heights, dims[axis_at] // blocks).reshape([-1 if axis == axis_at else 1 for axis in range(len(dims))])
    return factor_of


def rank_bounds(count, skew):
    weights = [(1 << 20) // math.isqrt(standing ** skew) + 1 for standing in range(1, count + 1)]
    width = 1 + sum(weights) // (1 << 30)
    return np.cumsum(np.array([max(1, weight // width) for weight in weights]))


def ranked_ids(stream_key, extent, number_of, skew):
    listing = rank_bounds(number_of, skew)
    pick = jax.random.randint(jax.random.fold_in(stream_key, 1), extent, 0, int(listing[number_of - 1]))
    rank = jnp.searchsorted(jnp.asarray(listing, jnp.int32), pick, side="right")
    return jax.random.permutation(jax.random.fold_in(stream_key, 2), number_of)[rank].astype(jnp.int32)


def gaussian(own_key, dims, scale, bound, split=(), kind=jnp.bfloat16):
    drawn = scale * jax.random.normal(own_key, dims, jnp.float32)
    if split:
        drawn = drawn * levels(own_key, dims, split, -0.22, 0.18)
    return jnp.clip(drawn, -bound, bound).astype(kind)


def setup_inputs(seed: int = 0, part: int = 0) -> dict:
    seeds = jax.random.split(jax.random.key(seed), 10)
    part_keys = jax.random.split(jax.random.fold_in(seeds[9], part), 10)
    tables = gaussian(seeds[0], (TABLES, VOCABULARY, WIDTH), 0.25, 1.5, ((0, 128),))
    bag_rows = with_ends(ranked_ids(part_keys[1], (N_DEV, TABLES, ROWS_MOST, POOLING), VOCABULARY, 2), jax.random.fold_in(part_keys[1], 3), 0, VOCABULARY - 1).astype(jnp.int32)
    bag_lengths = with_ends(jax.random.randint(part_keys[2], (N_DEV, TABLES, ROWS_MOST), 1, POOLING + 1), jax.random.fold_in(part_keys[2], 1), 1, POOLING).astype(jnp.int32)
    row_counts = draw_row_counts(jax.random.fold_in(jax.random.fold_in(seeds[9], part), 71), part)
    inverse = with_ends(jax.random.randint(part_keys[4], (BATCH, TABLES), 0, ROWS_MOST), jax.random.fold_in(part_keys[4], 1), 0, ROWS_MOST - 1).astype(jnp.int32)
    table_order = jax.random.permutation(seeds[5], TABLES).astype(jnp.int32)
    compress = gaussian(seeds[6], (COMPRESSED, TABLES), TABLES ** -0.5, 0.25)
    top_weight = gaussian(seeds[7], (TABLES * COMPRESSED, TOP_UNITS), (TABLES * COMPRESSED) ** -0.5, 0.0625)
    top_bias = gaussian(seeds[8], (TOP_UNITS,), 0.3, 1.8, (), jnp.float32)
    return {"tables": tables, "bag_rows": bag_rows, "bag_lengths": bag_lengths, "row_counts": row_counts, "inverse": inverse, "table_order": table_order, "compress": compress, "top_weight": top_weight, "top_bias": top_bias}


def pool_rows(tables, rows_here, lengths_here):
    gathered = jax.vmap(lambda one_table, one_bag: jnp.take(one_table, one_bag, axis=0))(tables, rows_here)
    active = jnp.arange(rows_here.shape[2], dtype=jnp.int32)[None, None, :] < lengths_here[..., None]
    summed = jnp.sum(jnp.where(active[..., None], gathered.astype(jnp.float32), jnp.zeros((), jnp.float32)), axis=2)
    return summed.astype(jnp.bfloat16)


def interact(features, compress, top_weight, top_bias):
    mixed = jnp.einsum("kf,bfe->bke", compress.astype(jnp.float32), features.astype(jnp.float32)).astype(jnp.bfloat16)
    pairwise = jnp.einsum("bfe,bke->bfk", features.astype(jnp.float32), mixed.astype(jnp.float32)).astype(jnp.bfloat16)
    hidden_pre = jnp.dot(pairwise.reshape(pairwise.shape[0], -1), top_weight, preferred_element_type=jnp.float32) + top_bias
    return jnp.maximum(hidden_pre, jnp.zeros((), jnp.float32)).astype(jnp.bfloat16)


def reference(tables, bag_rows, bag_lengths, row_counts, inverse, table_order, compress, top_weight, top_bias):
    slot_range = jnp.arange(TABLES, dtype=jnp.int32)
    matches = table_order[:, None] == slot_range[None, :]
    slot_of = jnp.sum(jnp.where(matches, slot_range[:, None], 0), axis=0).astype(jnp.int32)

    def one_device(device):
        rows_here = lax.dynamic_index_in_dim(bag_rows, device, 0, keepdims=False)
        lengths_here = lax.dynamic_index_in_dim(bag_lengths, device, 0, keepdims=False)
        counts_here = lax.dynamic_index_in_dim(row_counts, device, 0, keepdims=False)
        inverse_here = lax.dynamic_slice_in_dim(inverse, (device * BATCH_DEV).astype(jnp.int32), BATCH_DEV, 0)
        pooled = pool_rows(tables, rows_here, lengths_here)
        flat_rows = pooled.reshape(-1, WIDTH)
        positions = (slot_of[None, :] * ROWS_MOST + inverse_here).astype(jnp.int32)
        gathered = jnp.take(flat_rows, positions, axis=0)
        present = inverse_here < counts_here[slot_of][None, :]
        features = jnp.where(present[..., None], gathered, jnp.zeros((), jnp.bfloat16))
        return interact(features, compress, top_weight, top_bias)

    result = lax.map(one_device, jnp.arange(N_DEV, dtype=jnp.int32))
    return result.reshape(BATCH, TOP_UNITS)
```

```python
import functools

import jax
import jax.numpy as jnp
from jax import lax
from jax.experimental import pallas as pl
from jax.experimental.pallas import tpu as pltpu
from jax.sharding import PartitionSpec as P

PACK_ROOM = 80
GROUP = 4
UNROLL = 8


def pool_kernel(msg_ref, table_ref, out_ref, table_f32, packed, *, senders, most_rows, pool):
    vocab_rows = table_ref.shape[0]
    words = most_rows * pool // 2

    @pl.when(pl.program_id(0) == 0)
    def _():
        packed[...] = jnp.zeros_like(packed)
        table_f32[pl.ds(vocab_rows, 8), :] = jnp.zeros((8, table_f32.shape[1]), jnp.float32)

        def widen(i, carry):
            at = pl.multiple_of(i * 256, 256)
            table_f32[pl.ds(at, 256), :] = table_ref[pl.ds(at, 256), :].astype(jnp.float32)
            return carry

        lax.fori_loop(0, vocab_rows // 256, widen, 0)

    def one_sender(d, carry):
        start = jnp.int32(0)
        for slot in range(GROUP):
            count = msg_ref[d, GROUP * words + slot]

            def block(i, c, slot=slot, start=start):
                rows = []
                for r in range(UNROLL):
                    total = None
                    for h in range(pool // 2):
                        word = msg_ref[d, slot * words + h * most_rows + i * UNROLL + r]
                        low = table_f32[pl.ds(word & 0xFFFF, 1), :]
                        high = table_f32[pl.ds(lax.shift_right_logical(word, 16), 1), :]
                        part = low + high
                        total = part if total is None else total + part
                    rows.append(total)
                for r in range(UNROLL):
                    packed[pl.ds(start + i * UNROLL + r, 1), :] = rows[r]
                return c

            lax.fori_loop(0, lax.shift_right_logical(count + (UNROLL - 1), 3), block, 0)
            start = start + count
        out_ref[d] = packed[pl.ds(0, PACK_ROOM), :].astype(jnp.bfloat16)
        return carry

    lax.fori_loop(0, senders, one_sender, 0)


def pool_rows(message, table_rows, most_rows, pool):
    peers, width = message.shape
    senders = 8
    emb = table_rows.shape[1]
    return pl.pallas_call(
        functools.partial(pool_kernel, senders=senders, most_rows=most_rows, pool=pool),
        grid=(peers // senders,),
        out_shape=jax.ShapeDtypeStruct((peers, PACK_ROOM, emb), jnp.bfloat16),
        in_specs=[
            pl.BlockSpec((senders, width), lambda i: (i, 0), memory_space=pltpu.SMEM),
            pl.BlockSpec(table_rows.shape, lambda i: (0, 0)),
        ],
        out_specs=pl.BlockSpec((senders, PACK_ROOM, emb), lambda i: (i, 0, 0)),
        scratch_shapes=[
            pltpu.VMEM((table_rows.shape[0] + 8, emb), jnp.float32),
            pltpu.VMEM((PACK_ROOM + 32, emb), jnp.float32),
        ],
        compiler_params=pltpu.CompilerParams(vmem_limit_bytes=24 << 20),
        cost_estimate=pl.CostEstimate(flops=40_000_000_000, bytes_accessed=5 << 20, transcendentals=0),
    )(message, table_rows)


def tail_kernel(
    base_ref, row_ref, pos_ref, compress_ref, weight_ref, bias_ref, out_ref,
    rows_f32, feats, pairs, weight_vmem, weight_sem,
):
    total_rows, emb = row_ref.shape
    features, samples = pos_ref.shape
    mixes = compress_ref.shape[0]
    most_rows = rows_f32.shape[0] - total_rows
    copy = pltpu.make_async_copy(weight_ref, weight_vmem, weight_sem)
    copy.start()

    rows_f32[pl.ds(total_rows, most_rows), :] = jnp.zeros((most_rows, emb), jnp.float32)

    def widen(i, carry):
        at = pl.multiple_of(i * 256, 256)
        rows_f32[pl.ds(at, 256), :] = row_ref[pl.ds(at, 256), :].astype(jnp.float32)
        return carry

    lax.fori_loop(0, total_rows // 256, widen, 0)

    lane = lax.broadcasted_iota(jnp.int32, (16, 256), 1).astype(jnp.bfloat16)
    one = jnp.ones((16, 256), jnp.bfloat16)
    zero = jnp.zeros((16, 256), jnp.bfloat16)
    some = 32

    def expand(i, carry):
        at = pl.multiple_of(i * 16, 16)
        windows = []
        for half in range(2):
            parts = []
            for j in range(8):
                base = base_ref[i * 16 + half * 8 + j]
                parts.append(rows_f32[pl.ds(base, most_rows), :].astype(jnp.bfloat16))
            windows.append(jnp.concatenate(parts, axis=0))
        rhs = jnp.concatenate(windows, axis=1)
        pos = pos_ref[pl.ds(at, 16), :]
        for c in range(samples // some):
            picks = []
            for b in range(c * some, (c + 1) * some):
                wanted = jnp.broadcast_to(pos[:, b : b + 1], (16, 256))
                picks.append(jnp.where(wanted == lane, one, zero))
            lhs = jnp.concatenate(picks, axis=0)
            got = jnp.dot(lhs, rhs, preferred_element_type=jnp.float32)
            got = got.reshape(some, 2, 8, 2 * emb)
            both = jnp.concatenate([got[:, 0, :, :emb], got[:, 1, :, emb:]], axis=1)
            feats[pl.ds(c * some, some), pl.ds(at, 16), :] = both.astype(jnp.bfloat16)
        return carry

    lax.fori_loop(0, features // 16, expand, 0)

    per = 8

    def score(i, carry):
        mixing = compress_ref[...]
        stacks = []
        mixed = []
        for j in range(per // 2):
            b = i * per + 2 * j
            both = jnp.concatenate([feats[b], feats[b + 1]], axis=1)
            stacks.append(both)
            mixed.append(
                jnp.dot(mixing, both, preferred_element_type=jnp.float32).astype(jnp.bfloat16)
            )
        for j in range(per // 2):
            none = jnp.zeros((mixes, emb), jnp.bfloat16)
            first = jnp.concatenate([mixed[j][:, :emb], none], axis=1)
            second = jnp.concatenate([none, mixed[j][:, emb:]], axis=1)
            lhs = jnp.concatenate([first, second], axis=0)
            got = lax.dot_general(
                lhs, stacks[j], (((1,), (1,)), ((), ())), preferred_element_type=jnp.float32
            )
            at = pl.multiple_of((i * per + 2 * j) * mixes, 2 * mixes)
            for c in range(features // 128):
                pairs[c, pl.ds(at, 2 * mixes), :] = got[:, c * 128 : (c + 1) * 128]
        return carry

    lax.fori_loop(0, samples // per, score, 0)

    copy.wait()
    total = jnp.broadcast_to(bias_ref[...], (samples, out_ref.shape[1]))
    for k in range(mixes):
        lhs = jnp.concatenate(
            [pairs[c, pl.ds(k, samples, stride=mixes), :] for c in range(features // 128)], axis=1
        ).astype(jnp.bfloat16)
        total = total + jnp.dot(lhs, weight_vmem[k], preferred_element_type=jnp.float32)
    out_ref[...] = jnp.maximum(total, 0.0).astype(jnp.bfloat16)


def score_samples(base, rows, pos, compress, weight, bias, most_rows):
    features, samples = pos.shape
    mixes = compress.shape[0]
    units = weight.shape[2]
    emb = rows.shape[1]
    vmem = pl.BlockSpec(memory_space=pltpu.VMEM)
    return pl.pallas_call(
        tail_kernel,
        out_shape=jax.ShapeDtypeStruct((samples, units), jnp.bfloat16),
        in_specs=[
            pl.BlockSpec(memory_space=pltpu.SMEM), vmem, vmem, vmem,
            pl.BlockSpec(memory_space=pltpu.HBM), vmem,
        ],
        out_specs=vmem,
        scratch_shapes=[
            pltpu.VMEM((rows.shape[0] + most_rows, emb), jnp.float32),
            pltpu.VMEM((samples, features, emb), jnp.bfloat16),
            pltpu.VMEM((features // 128, samples * mixes, 128), jnp.float32),
            pltpu.VMEM(weight.shape, jnp.bfloat16),
            pltpu.SemaphoreType.DMA(()),
        ],
        compiler_params=pltpu.CompilerParams(vmem_limit_bytes=60 << 20),
        cost_estimate=pl.CostEstimate(flops=20_000_000_000, bytes_accessed=16 << 20, transcendentals=0),
    )(base, rows, pos, compress, weight, bias)


def bag_message(bag_rows, bag_lengths, counts, vocabulary):
    slots, most_rows, pool = bag_rows.shape
    ids = jnp.transpose(bag_rows, (1, 2, 0))
    lengths = jnp.transpose(bag_lengths, (1, 0))
    offset = (jnp.arange(slots, dtype=jnp.int32) % GROUP) * vocabulary
    spare = GROUP * vocabulary
    words = []
    for h in range(pool // 2):
        low = jnp.where(2 * h < lengths, ids[:, 2 * h, :] + offset[None, :], spare)
        high = jnp.where(2 * h + 1 < lengths, ids[:, 2 * h + 1, :] + offset[None, :], spare)
        words.append(low | (high << 16))
    packed = jnp.concatenate(words, axis=0)
    packed = jnp.transpose(packed, (1, 0)).reshape(slots // GROUP, -1)
    fill = (-(packed.shape[1] + GROUP)) % 128
    counts = jnp.pad(counts.reshape(-1, GROUP), ((0, 0), (0, fill)))
    return jnp.concatenate([packed, counts], axis=1)


def shards(
    tables, bag_rows, bag_lengths, row_counts, inverse, table_order, compress, top_weight, top_bias
):
    local_tables, vocabulary, emb = tables.shape
    slots = table_order.shape[0]
    most_rows, pool = bag_rows.shape[2:]
    mixes = compress.shape[0]
    counts = row_counts[0]
    message = bag_message(bag_rows[0], bag_lengths[0], counts, vocabulary)
    got = lax.all_to_all(message, "dev", split_axis=0, concat_axis=0, tiled=True)
    pooled = pool_rows(got, tables.reshape(-1, emb), most_rows, pool)
    arrived = lax.all_to_all(pooled, "dev", split_axis=0, concat_axis=0, tiled=True)

    grouped = counts.reshape(-1, GROUP)
    before = jnp.cumsum(grouped, axis=1) - grouped
    group_at = jnp.arange(slots // GROUP, dtype=jnp.int32)[:, None] * PACK_ROOM
    slot_base = (before + group_at).reshape(-1)
    slot_range = jnp.arange(slots, dtype=jnp.int32)
    matches = table_order[:, None] == slot_range[None, :]
    feature_base = jnp.sum(jnp.where(matches, slot_base[:, None], 0), axis=0)
    feature_count = jnp.sum(jnp.where(matches, counts[:, None], 0), axis=0)
    shift = (slot_range % 8) * most_rows
    pos = jnp.where(inverse < feature_count[None, :], inverse + shift[None, :], -1)
    pos = jnp.transpose(pos.astype(jnp.bfloat16), (1, 0))
    weight = jnp.transpose(top_weight.reshape(slots, mixes, -1), (1, 0, 2))
    return score_samples(
        feature_base, arrived.reshape(-1, emb), pos, compress, weight, top_bias[None, :], most_rows
    )


def solution(mesh):
    return jax.shard_map(
        shards,
        mesh=mesh,
        in_specs=(
            P("dev", None, None),
            P(("rep", "dev"), None, None, None),
            P(("rep", "dev"), None, None),
            P(("rep", "dev"), None),
            P(("rep", "dev"), None),
            P(),
            P(),
            P(),
            P(),
        ),
        out_specs=P(("rep", "dev"), None),
        check_vma=False,
    )
```

```python
import functools

import jax
import jax.numpy as jnp
from jax import lax
from jax.experimental import pallas as pl
from jax.experimental.pallas import tpu as pltpu
from jax.sharding import PartitionSpec as P

PACK_ROOM = 80
CHUNKS = ((0, 16), (16, 64))
BLOCK = 8
PARTS = 4
GROUP = 4


def message_kernel(ids_ref, lengths_ref, counts_ref, out_ref, words, *, vocabulary):
    most_rows, pool, slots = ids_ref.shape
    spare = GROUP * vocabulary
    slot = lax.broadcasted_iota(jnp.int32, (8, slots), 1) % GROUP
    counts = jnp.broadcast_to(counts_ref[...], (8, slots))
    offset = jnp.zeros((8, slots), jnp.int32)
    for back in range(1, GROUP):
        offset = offset + jnp.where(slot >= back, pltpu.roll(counts, back, 1), 0)
    offset = offset[:1, :]
    table = slot[:1, :] * vocabulary
    lengths = lengths_ref[...]
    used = lax.broadcasted_iota(jnp.int32, (most_rows, slots), 0) < counts[:1, :]
    room = 128
    for h in range(pool // 2):
        low = jnp.where(2 * h < lengths, ids_ref[:, 2 * h, :] + table, spare)
        high = jnp.where(2 * h + 1 < lengths, ids_ref[:, 2 * h + 1, :] + table, spare)
        word = jnp.where(used, low | (high << 16), 0)
        word = jnp.concatenate([word, jnp.zeros((8, slots), jnp.int32)], axis=0)
        for bit in range(3):
            moved = pltpu.roll(word, 1 << bit, 0)
            word = jnp.where(((offset >> bit) & 1) == 1, moved, word)
        word = jnp.concatenate(
            [word, jnp.zeros((room - word.shape[0], slots), jnp.int32)], axis=0
        )
        for bit in range(3, 7):
            by = 1 << bit
            moved = jnp.concatenate(
                [jnp.zeros((by, slots), jnp.int32), word[: room - by, :]], axis=0
            )
            word = jnp.where(((offset >> bit) & 1) == 1, moved, word)
        words[...] = jnp.transpose(word, (1, 0))
        groups = slots // GROUP
        total = words[pl.ds(0, groups, stride=GROUP), :]
        for member in range(1, GROUP):
            total = total + words[pl.ds(member, groups, stride=GROUP), :]
        out_ref[pl.ds(h, groups, stride=pool // 2), :] = total


def bag_message(bag_rows, bag_lengths, counts, vocabulary):
    slots, most_rows, pool = bag_rows.shape
    groups = slots // GROUP
    message = pl.pallas_call(
        functools.partial(message_kernel, vocabulary=vocabulary),
        out_shape=jax.ShapeDtypeStruct((groups * pool // 2, 128), jnp.int32),
        in_specs=[pl.BlockSpec(memory_space=pltpu.VMEM)] * 3,
        out_specs=pl.BlockSpec(memory_space=pltpu.VMEM),
        scratch_shapes=[pltpu.VMEM((slots, 128), jnp.int32)],
    )(jnp.transpose(bag_rows, (1, 2, 0)), jnp.transpose(bag_lengths, (1, 0)), counts)
    return message.reshape(groups, pool // 2, 128)


def pool_kernel(
    msg_ref, table_ref, out_ref, table_f32, pooled, ids, ids_smem, sems, *, first, rows, pool
):
    vocab_rows, emb = table_ref.shape
    peers = out_ref.shape[0]
    lanes = ids.shape[1]
    per = min(pool, lanes // rows)
    lines = pool // per
    shares = sems.shape[0]
    lane = lax.broadcasted_iota(jnp.int32, (peers, lanes), 1)
    held = []
    for h in range(pool // 2):
        word = msg_ref[pl.ds(h, peers, stride=pool // 2), :]
        held += [word & 0xFFFF, lax.shift_right_logical(word, 16)]
    for q in range(lines):
        line = jnp.zeros((peers, lanes), jnp.int32)
        for r in range(per):
            moved = pltpu.roll(held[q * per + r], (r * rows - first) % lanes, 1)
            line = jnp.where((lane >= r * rows) & (lane < (r + 1) * rows), moved, line)
        ids[pl.ds(q, peers, stride=lines), :] = line
    step = peers // shares
    copies = [
        pltpu.make_async_copy(
            ids.at[pl.ds(c * step * lines, step * lines)],
            ids_smem.at[pl.ds(c * step * lines, step * lines)],
            sems.at[c],
        )
        for c in range(shares)
    ]
    for copy in copies:
        copy.start()
    table_f32[pl.ds(vocab_rows, 8), :] = jnp.zeros((8, emb), jnp.float32)

    def widen(i, carry):
        at = pl.multiple_of(i * 256, 256)
        table_f32[pl.ds(at, 256), :] = table_ref[pl.ds(at, 256), :].astype(jnp.float32)
        return carry

    lax.fori_loop(0, vocab_rows // 256, widen, 0)

    def one_sender(d, carry):
        views = [ids_smem.at[pl.ds(d * lines + q, 1)] for q in range(lines)]
        for j in range(rows):
            parts = [
                table_f32[pl.ds(views[p // per][0, (p % per) * rows + j], 1), :]
                for p in range(pool)
            ]
            while len(parts) > 1:
                parts = [parts[i] + parts[i + 1] for i in range(0, len(parts), 2)]
            pooled[pl.ds(d * rows + j, 1), :] = parts[0]
        return carry

    for c in range(shares):
        copies[c].wait()
        lax.fori_loop(c * step, (c + 1) * step, one_sender, 0)

    def narrow(d, carry):
        at = pl.multiple_of(d * rows, 8)
        out_ref[d] = pooled[pl.ds(at, rows), :].astype(jnp.bfloat16)
        return carry

    lax.fori_loop(0, peers, narrow, 0, unroll=4)


def pool_rows(message, table_rows, first, rows):
    peers, halves, width = message.shape
    pool = 2 * halves
    lines = pool // min(pool, width // rows)
    emb = table_rows.shape[1]
    vmem = pl.BlockSpec(memory_space=pltpu.VMEM)
    return pl.pallas_call(
        functools.partial(pool_kernel, first=first, rows=rows, pool=pool),
        out_shape=jax.ShapeDtypeStruct((peers, rows, emb), jnp.bfloat16),
        in_specs=[vmem, vmem],
        out_specs=vmem,
        scratch_shapes=[
            pltpu.VMEM((table_rows.shape[0] + 8, emb), jnp.float32),
            pltpu.VMEM((peers * rows, emb), jnp.float32),
            pltpu.VMEM((peers * lines, width), jnp.int32),
            pltpu.SMEM((peers * lines, width), jnp.int32),
            pltpu.SemaphoreType.DMA((4,)),
        ],
        compiler_params=pltpu.CompilerParams(vmem_limit_bytes=24 << 20),
        cost_estimate=pl.CostEstimate(flops=20_000_000_000, bytes_accessed=5 << 20, transcendentals=0),
    )(message.reshape(peers * halves, width), table_rows)


def selector_kernel(pos_ref, out_ref):
    blocks, rows, lanes = out_ref.shape
    samples = rows // BLOCK
    lane = lax.broadcasted_iota(jnp.int32, (BLOCK, lanes), 1).astype(jnp.float32)

    def one_block(i, carry):
        pos = pos_ref[pl.ds(pl.multiple_of(i * BLOCK, BLOCK), BLOCK), :]
        for b in range(0, samples, 2):
            pair = [
                jnp.where(jnp.broadcast_to(pos[:, c : c + 1], (BLOCK, lanes)) == lane, 1.0, 0.0)
                for c in (b, b + 1)
            ]
            out_ref[i, pl.ds(b * BLOCK, 2 * BLOCK), :] = jnp.concatenate(pair, axis=0).astype(
                jnp.bfloat16
            )
        return carry

    lax.fori_loop(0, blocks, one_block, 0)


def build_selectors(pos):
    features, samples = pos.shape
    blocks = features // BLOCK
    some = 4
    return pl.pallas_call(
        selector_kernel,
        grid=(blocks // some,),
        out_shape=jax.ShapeDtypeStruct((blocks, samples * BLOCK, 128), jnp.bfloat16),
        in_specs=[pl.BlockSpec((some * BLOCK, samples), lambda i: (i, 0))],
        out_specs=pl.BlockSpec((some, samples * BLOCK, 128), lambda i: (i, 0, 0)),
        compiler_params=pltpu.CompilerParams(vmem_limit_bytes=8 << 20),
        cost_estimate=pl.CostEstimate(flops=10_000_000_000, bytes_accessed=16 << 20, transcendentals=0),
    )(pos)


def tail_kernel(base_ref, selector_ref, compress_ref, weight_ref, bias_ref, *refs, most_rows):
    row_refs = refs[: len(CHUNKS)]
    (
        out_ref, rows_f32, feats, pairs, select_vmem, weight_vmem, select_sem, weight_sem,
    ) = refs[len(CHUNKS) :]
    groups, _, emb = row_refs[0].shape
    total_rows = groups * PACK_ROOM
    samples, features, _ = feats.shape
    mixes = compress_ref.shape[0]
    blocks = features // BLOCK
    share = blocks // PARTS
    copies = [
        pltpu.make_async_copy(
            selector_ref.at[pl.ds(part * share, share)],
            select_vmem.at[pl.ds(part * share, share)],
            select_sem.at[part],
        )
        for part in range(PARTS)
    ]
    for copy in copies:
        copy.start()
    weight_copy = pltpu.make_async_copy(weight_ref, weight_vmem, weight_sem)
    weight_copy.start()

    rows_f32[pl.ds(total_rows, most_rows), :] = jnp.zeros((most_rows, emb), jnp.float32)

    def widen(g, carry):
        for (first, count), row_ref in zip(CHUNKS, row_refs):
            at = pl.multiple_of(g * PACK_ROOM + first, 16)
            rows_f32[pl.ds(at, count), :] = row_ref[g].astype(jnp.float32)
        return carry

    lax.fori_loop(0, groups, widen, 0, unroll=4)

    first_half = lax.broadcasted_iota(jnp.int32, (1, BLOCK, emb), 1) < BLOCK // 2
    some = 32

    def expand(i, carry):
        for pair in range(2):
            tops = []
            for half in range(2):
                block = 4 * i + 2 * pair + half
                sides = []
                for side in range(2):
                    parts = []
                    for j in range(BLOCK // 2):
                        base = base_ref[block * BLOCK + side * (BLOCK // 2) + j]
                        parts.append(rows_f32[pl.ds(base, most_rows), :].astype(jnp.bfloat16))
                    sides.append(jnp.concatenate(parts, axis=0))
                tops.append((block, jnp.concatenate(sides, axis=1)))
            at = pl.multiple_of((4 * i + 2 * pair) * BLOCK, 2 * BLOCK)
            for c in range(samples // some):
                halves = []
                for block, rhs in tops:
                    lhs = select_vmem[block, pl.ds(c * some * BLOCK, some * BLOCK), :]
                    got = jnp.dot(lhs, rhs, preferred_element_type=jnp.float32)
                    got = got.reshape(some, BLOCK, 2 * emb)
                    halves.append(jnp.where(first_half, got[:, :, :emb], got[:, :, emb:]))
                both = jnp.concatenate(halves, axis=1)
                feats[pl.ds(c * some, some), pl.ds(at, 2 * BLOCK), :] = both.astype(jnp.bfloat16)
        return carry

    for part in range(PARTS):
        copies[part].wait()
        lax.fori_loop(part * share // 4, (part + 1) * share // 4, expand, 0)

    per = 8

    def score(i, carry):
        mixing = compress_ref[...]
        stacks = []
        mixed = []
        for j in range(per // 2):
            b = i * per + 2 * j
            both = jnp.concatenate([feats[b], feats[b + 1]], axis=1)
            stacks.append(both)
            mixed.append(
                jnp.dot(mixing, both, preferred_element_type=jnp.float32).astype(jnp.bfloat16)
            )
        for j in range(per // 2):
            none = jnp.zeros((mixes, emb), jnp.bfloat16)
            first = jnp.concatenate([mixed[j][:, :emb], none], axis=1)
            second = jnp.concatenate([none, mixed[j][:, emb:]], axis=1)
            lhs = jnp.concatenate([first, second], axis=0)
            got = jnp.dot(lhs, jnp.transpose(stacks[j]), preferred_element_type=jnp.float32)
            at = pl.multiple_of((i * per + 2 * j) * mixes, 2 * mixes)
            for c in range(features // 128):
                pairs[c, pl.ds(at, 2 * mixes), :] = got[:, c * 128 : (c + 1) * 128]
        return carry

    lax.fori_loop(0, samples // per, score, 0)

    weight_copy.wait()
    total = jnp.broadcast_to(bias_ref[...], (samples, out_ref.shape[1]))
    for k in range(mixes):
        lhs = jnp.concatenate(
            [pairs[c, pl.ds(k, samples, stride=mixes), :] for c in range(features // 128)], axis=1
        ).astype(jnp.bfloat16)
        total = total + jnp.dot(lhs, weight_vmem[k], preferred_element_type=jnp.float32)
    out_ref[...] = jnp.maximum(total, 0.0).astype(jnp.bfloat16)


def score_samples(base, selectors, arrived, compress, weight, bias, most_rows):
    mixes, features = compress.shape
    units = weight.shape[2]
    groups, _, emb = arrived[0].shape
    samples = selectors.shape[1] // BLOCK
    vmem = pl.BlockSpec(memory_space=pltpu.VMEM)
    hbm = pl.BlockSpec(memory_space=pltpu.HBM)
    return pl.pallas_call(
        functools.partial(tail_kernel, most_rows=most_rows),
        out_shape=jax.ShapeDtypeStruct((samples, units), jnp.bfloat16),
        in_specs=[pl.BlockSpec(memory_space=pltpu.SMEM), hbm, vmem, hbm, vmem]
        + [vmem] * len(arrived),
        out_specs=vmem,
        scratch_shapes=[
            pltpu.VMEM((groups * PACK_ROOM + most_rows, emb), jnp.float32),
            pltpu.VMEM((samples, features, emb), jnp.bfloat16),
            pltpu.VMEM((features // 128, samples * mixes, 128), jnp.float32),
            pltpu.VMEM(selectors.shape, jnp.bfloat16),
            pltpu.VMEM(weight.shape, jnp.bfloat16),
            pltpu.SemaphoreType.DMA((PARTS,)),
            pltpu.SemaphoreType.DMA(()),
        ],
        compiler_params=pltpu.CompilerParams(vmem_limit_bytes=53 << 20),
        cost_estimate=pl.CostEstimate(flops=20_000_000_000, bytes_accessed=16 << 20, transcendentals=0),
    )(base, selectors, compress, weight, bias, *arrived)


def shards(
    tables, bag_rows, bag_lengths, row_counts, inverse, table_order, compress, top_weight, top_bias
):
    vocabulary, emb = tables.shape[1:]
    slots = table_order.shape[0]
    most_rows = bag_rows.shape[2]
    mixes = compress.shape[0]
    counts = row_counts[0]
    message = bag_message(bag_rows[0], bag_lengths[0], row_counts, vocabulary)
    got = lax.all_to_all(message, "dev", split_axis=0, concat_axis=0, tiled=True)
    table_rows = tables.reshape(-1, emb)
    arrived = []
    for first, count in CHUNKS:
        pooled = pool_rows(got, table_rows, first, count)
        arrived.append(lax.all_to_all(pooled, "dev", split_axis=0, concat_axis=0, tiled=True))

    grouped = counts.reshape(-1, GROUP)
    before = jnp.cumsum(grouped, axis=1) - grouped
    group_at = jnp.arange(slots // GROUP, dtype=jnp.int32)[:, None] * PACK_ROOM
    slot_base = (before + group_at).reshape(-1)
    slot_range = jnp.arange(slots, dtype=jnp.int32)
    matches = table_order[:, None] == slot_range[None, :]
    feature_base = jnp.sum(jnp.where(matches, slot_base[:, None], 0), axis=0)
    feature_count = jnp.sum(jnp.where(matches, counts[:, None], 0), axis=0)
    shift = (slot_range % (BLOCK // 2)) * most_rows
    pos = jnp.where(inverse < feature_count[None, :], inverse + shift[None, :], -1)
    selectors = build_selectors(jnp.transpose(pos.astype(jnp.float32), (1, 0)))
    weight = jnp.transpose(top_weight.reshape(slots, mixes, -1), (1, 0, 2))
    return score_samples(
        feature_base, selectors, arrived, compress, weight, top_bias[None, :], most_rows
    )


def solution(mesh):
    return jax.shard_map(
        shards,
        mesh=mesh,
        in_specs=(
            P("dev", None, None),
            P(("rep", "dev"), None, None, None),
            P(("rep", "dev"), None, None),
            P(("rep", "dev"), None),
            P(("rep", "dev"), None),
            P(),
            P(),
            P(),
            P(),
        ),
        out_specs=P(("rep", "dev"), None),
        check_vma=False,
    )
```

```python
import functools

import jax
import jax.numpy as jnp
from jax import lax
from jax.experimental import pallas as pl
from jax.experimental.pallas import tpu as pltpu
from jax.sharding import PartitionSpec as P

PACK_ROOM = 80
CHUNKS = ((0, 80),)
BLOCK = 8
PARTS = 4
GROUP = 4


def message_kernel(ids_ref, lengths_ref, counts_ref, out_ref, words, *, vocabulary):
    most_rows, pool, slots = ids_ref.shape
    spare = GROUP * vocabulary
    slot = lax.broadcasted_iota(jnp.int32, (8, slots), 1) % GROUP
    counts = jnp.broadcast_to(counts_ref[...], (8, slots))
    offset = jnp.zeros((8, slots), jnp.int32)
    for back in range(1, GROUP):
        offset = offset + jnp.where(slot >= back, pltpu.roll(counts, back, 1), 0)
    offset = offset[:1, :]
    table = slot[:1, :] * vocabulary
    lengths = lengths_ref[...]
    used = lax.broadcasted_iota(jnp.int32, (most_rows, slots), 0) < counts[:1, :]
    room = 128
    for h in range(pool // 2):
        low = jnp.where(2 * h < lengths, ids_ref[:, 2 * h, :] + table, spare)
        high = jnp.where(2 * h + 1 < lengths, ids_ref[:, 2 * h + 1, :] + table, spare)
        word = jnp.where(used, low | (high << 16), 0)
        word = jnp.concatenate([word, jnp.zeros((8, slots), jnp.int32)], axis=0)
        for bit in range(3):
            moved = pltpu.roll(word, 1 << bit, 0)
            word = jnp.where(((offset >> bit) & 1) == 1, moved, word)
        word = jnp.concatenate(
            [word, jnp.zeros((room - word.shape[0], slots), jnp.int32)], axis=0
        )
        for bit in range(3, 7):
            by = 1 << bit
            moved = jnp.concatenate(
                [jnp.zeros((by, slots), jnp.int32), word[: room - by, :]], axis=0
            )
            word = jnp.where(((offset >> bit) & 1) == 1, moved, word)
        words[...] = jnp.transpose(word, (1, 0))
        groups = slots // GROUP
        total = words[pl.ds(0, groups, stride=GROUP), :]
        for member in range(1, GROUP):
            total = total + words[pl.ds(member, groups, stride=GROUP), :]
        out_ref[pl.ds(h, groups, stride=pool // 2), :] = total


def bag_message(bag_rows, bag_lengths, counts, vocabulary):
    slots, most_rows, pool = bag_rows.shape
    groups = slots // GROUP
    message = pl.pallas_call(
        functools.partial(message_kernel, vocabulary=vocabulary),
        out_shape=jax.ShapeDtypeStruct((groups * pool // 2, 128), jnp.int32),
        in_specs=[pl.BlockSpec(memory_space=pltpu.VMEM)] * 3,
        out_specs=pl.BlockSpec(memory_space=pltpu.VMEM),
        scratch_shapes=[pltpu.VMEM((slots, 128), jnp.int32)],
    )(jnp.transpose(bag_rows, (1, 2, 0)), jnp.transpose(bag_lengths, (1, 0)), counts)
    return message.reshape(groups, pool // 2, 128)


def pool_kernel(
    msg_ref, table_hbm, out_ref, table_ref, table_f32, pooled, ids, ids_smem, sems, table_sem,
    *, first, rows, pool,
):
    vocab_rows, emb = table_hbm.shape
    table_copy = pltpu.make_async_copy(table_hbm, table_ref, table_sem)
    table_copy.start()
    peers = out_ref.shape[0]
    lanes = ids.shape[1]
    per = min(pool, lanes // rows)
    lines = -(-pool // per)
    shares = sems.shape[0]
    lane = lax.broadcasted_iota(jnp.int32, (peers, lanes), 1)
    held = []
    for h in range(pool // 2):
        word = msg_ref[pl.ds(h, peers, stride=pool // 2), :]
        held += [word & 0xFFFF, lax.shift_right_logical(word, 16)]
    for q in range(lines):
        line = jnp.zeros((peers, lanes), jnp.int32)
        for r in range(per):
            moved = pltpu.roll(held[q * per + r], (r * rows - first) % lanes, 1)
            line = jnp.where((lane >= r * rows) & (lane < (r + 1) * rows), moved, line)
        ids[pl.ds(q, peers, stride=lines), :] = line
    step = peers // shares
    copies = [
        pltpu.make_async_copy(
            ids.at[pl.ds(c * step * lines, step * lines)],
            ids_smem.at[pl.ds(c * step * lines, step * lines)],
            sems.at[c],
        )
        for c in range(shares)
    ]
    for copy in copies:
        copy.start()
    table_f32[pl.ds(vocab_rows, 8), :] = jnp.zeros((8, emb), jnp.float32)
    table_copy.wait()

    def widen(i, carry):
        at = pl.multiple_of(i * 256, 256)
        table_f32[pl.ds(at, 256), :] = table_ref[pl.ds(at, 256), :].astype(jnp.float32)
        return carry

    lax.fori_loop(0, vocab_rows // 256, widen, 0)

    def one_sender(d, carry):
        views = [ids_smem.at[pl.ds(d * lines + q, 1)] for q in range(lines)]
        for j in range(rows):
            parts = [
                table_f32[pl.ds(views[p // per][0, (p % per) * rows + j], 1), :]
                for p in range(pool)
            ]
            while len(parts) > 1:
                parts = [parts[i] + parts[i + 1] for i in range(0, len(parts), 2)]
            pooled[pl.ds(d * rows + j, 1), :] = parts[0]
        return carry

    for c in range(shares):
        copies[c].wait()
        lax.fori_loop(c * step, (c + 1) * step, one_sender, 0)

    def narrow(d, carry):
        at = pl.multiple_of(d * rows, 8)
        out_ref[d] = pooled[pl.ds(at, rows), :].astype(jnp.bfloat16)
        return carry

    lax.fori_loop(0, peers, narrow, 0, unroll=4)


def pool_rows(message, table_rows, first, rows):
    peers, halves, width = message.shape
    pool = 2 * halves
    lines = -(-pool // min(pool, width // rows))
    emb = table_rows.shape[1]
    vmem = pl.BlockSpec(memory_space=pltpu.VMEM)
    return pl.pallas_call(
        functools.partial(pool_kernel, first=first, rows=rows, pool=pool),
        out_shape=jax.ShapeDtypeStruct((peers, rows, emb), jnp.bfloat16),
        in_specs=[vmem, pl.BlockSpec(memory_space=pltpu.HBM)],
        out_specs=vmem,
        scratch_shapes=[
            pltpu.VMEM(table_rows.shape, jnp.bfloat16),
            pltpu.VMEM((table_rows.shape[0] + 8, emb), jnp.float32),
            pltpu.VMEM((peers * rows, emb), jnp.float32),
            pltpu.VMEM((peers * lines, width), jnp.int32),
            pltpu.SMEM((peers * lines, width), jnp.int32),
            pltpu.SemaphoreType.DMA((4,)),
            pltpu.SemaphoreType.DMA(()),
        ],
        compiler_params=pltpu.CompilerParams(vmem_limit_bytes=24 << 20),
        cost_estimate=pl.CostEstimate(flops=20_000_000_000, bytes_accessed=5 << 20, transcendentals=0),
    )(message.reshape(peers * halves, width), table_rows)


def selector_kernel(pos_ref, out_ref):
    blocks, rows, lanes = out_ref.shape
    pairs = rows // BLOCK
    half = lanes // 2
    lane = lax.broadcasted_iota(jnp.int32, (BLOCK, half), 1).astype(jnp.float32)
    upper = lax.broadcasted_iota(jnp.int32, (BLOCK, pos_ref.shape[1]), 0) < BLOCK // 2

    def one_block(i, carry):
        here = pos_ref[pl.ds(pl.multiple_of(i * BLOCK, BLOCK), BLOCK), :]
        swapped = pltpu.roll(here, BLOCK // 2, 0)
        samples = here.shape[1]
        sides = (
            jnp.where(upper, here, pltpu.roll(swapped, samples - 1, 1)),
            jnp.where(upper, swapped, pltpu.roll(here, samples - 1, 1)),
        )
        for side, pos in enumerate(sides):
            for p in range(0, pairs, 2):
                both = [
                    jnp.where(jnp.broadcast_to(pos[:, c : c + 1], (BLOCK, half)) == lane, 1.0, 0.0)
                    for c in (2 * p, 2 * p + 2)
                ]
                out_ref[i, pl.ds(p * BLOCK, 2 * BLOCK), pl.ds(side * half, half)] = (
                    jnp.concatenate(both, axis=0).astype(jnp.bfloat16)
                )
        return carry

    lax.fori_loop(0, blocks, one_block, 0)


def build_selectors(pos):
    features, samples = pos.shape
    blocks = features // BLOCK
    pairs = samples // 2
    some = 4
    return pl.pallas_call(
        selector_kernel,
        grid=(blocks // some,),
        out_shape=jax.ShapeDtypeStruct((blocks, pairs * BLOCK, 256), jnp.bfloat16),
        in_specs=[pl.BlockSpec((some * BLOCK, samples), lambda i: (i, 0))],
        out_specs=pl.BlockSpec((some, pairs * BLOCK, 256), lambda i: (i, 0, 0)),
        compiler_params=pltpu.CompilerParams(vmem_limit_bytes=8 << 20),
        cost_estimate=pl.CostEstimate(flops=10_000_000_000, bytes_accessed=16 << 20, transcendentals=0),
    )(pos)


def tail_kernel(base_ref, selector_ref, compress_ref, weight_ref, bias_ref, *refs, most_rows):
    row_refs = refs[: len(CHUNKS)]
    (
        out_ref, rows_f32, feats, pairs, turned, select_vmem, weight_vmem, select_sem, weight_sem,
    ) = refs[len(CHUNKS) :]
    groups, _, emb = row_refs[0].shape
    total_rows = groups * PACK_ROOM
    sample_pairs, _, features, _ = feats.shape
    samples = 2 * sample_pairs
    mixes = compress_ref.shape[0]
    blocks = features // BLOCK
    share = blocks // PARTS
    copies = [
        pltpu.make_async_copy(
            selector_ref.at[pl.ds(part * share, share)],
            select_vmem.at[pl.ds(part * share, share)],
            select_sem.at[part],
        )
        for part in range(PARTS)
    ]
    for copy in copies:
        copy.start()
    weight_copy = pltpu.make_async_copy(weight_ref, weight_vmem, weight_sem)
    weight_copy.start()

    rows_f32[pl.ds(total_rows, most_rows), :] = jnp.zeros((most_rows, emb), jnp.float32)

    def widen(g, carry):
        for (first, count), row_ref in zip(CHUNKS, row_refs):
            at = pl.multiple_of(g * PACK_ROOM + first, 16)
            rows_f32[pl.ds(at, count), :] = row_ref[g].astype(jnp.float32)
        return carry

    lax.fori_loop(0, groups, widen, 0, unroll=4)

    first_half = lax.broadcasted_iota(jnp.int32, (1, BLOCK, emb), 1) < BLOCK // 2
    some = 32
    empty = jnp.zeros((BLOCK // 2 * most_rows, emb), jnp.bfloat16)

    def expand(i, carry):
        for pair in range(2):
            tops = []
            for half in range(2):
                block = 4 * i + 2 * pair + half
                sides = []
                for side in range(2):
                    parts = []
                    for j in range(BLOCK // 2):
                        base = base_ref[block * BLOCK + side * (BLOCK // 2) + j]
                        parts.append(rows_f32[pl.ds(base, most_rows), :].astype(jnp.bfloat16))
                    sides.append(jnp.concatenate(parts, axis=0))
                top = jnp.concatenate([sides[0], empty], axis=1)
                bottom = jnp.concatenate([empty, sides[1]], axis=1)
                tops.append((block, jnp.concatenate([top, bottom], axis=0)))
            at = pl.multiple_of((4 * i + 2 * pair) * BLOCK, 2 * BLOCK)
            for c in range(sample_pairs // some):
                even, odd = [], []
                for block, rhs in tops:
                    lhs = select_vmem[block, pl.ds(c * some * BLOCK, some * BLOCK), :]
                    got = jnp.dot(lhs, rhs, preferred_element_type=jnp.float32)
                    got = got.reshape(some, BLOCK, 2 * emb)
                    left, right = got[:, :, :emb], got[:, :, emb:]
                    even.append(jnp.where(first_half, left, pltpu.roll(right, BLOCK // 2, 1)))
                    odd.append(jnp.where(first_half, pltpu.roll(left, BLOCK // 2, 1), right))
                for which, parts in enumerate((even, odd)):
                    feats[pl.ds(c * some, some), which, pl.ds(at, 2 * BLOCK), :] = jnp.concatenate(
                        parts, axis=1
                    ).astype(jnp.bfloat16)
        return carry

    for part in range(PARTS):
        copies[part].wait()
        lax.fori_loop(part * share // 4, (part + 1) * share // 4, expand, 0)

    per = 8

    def score(i, carry):
        mixing = compress_ref[...]
        mixed = []
        for j in range(per // 2):
            at = i * (per // 2) + j
            both = jnp.concatenate([feats[at, 0], feats[at, 1]], axis=1)
            turned[j] = jnp.transpose(both)
            mixed.append(
                jnp.dot(mixing, both, preferred_element_type=jnp.float32).astype(jnp.bfloat16)
            )
        for j in range(per // 2):
            none = jnp.zeros((mixes, emb), jnp.bfloat16)
            first = jnp.concatenate([mixed[j][:, :emb], none], axis=1)
            second = jnp.concatenate([none, mixed[j][:, emb:]], axis=1)
            lhs = jnp.concatenate([first, second], axis=0)
            got = jnp.dot(lhs, turned[j], preferred_element_type=jnp.float32)
            at = pl.multiple_of((i * per + 2 * j) * mixes, 2 * mixes)
            for c in range(features // 128):
                pairs[c, pl.ds(at, 2 * mixes), :] = got[:, c * 128 : (c + 1) * 128]
        return carry

    lax.fori_loop(0, samples // per, score, 0)

    weight_copy.wait()
    total = jnp.broadcast_to(bias_ref[...], (samples, out_ref.shape[1]))
    for k in range(mixes):
        lhs = jnp.concatenate(
            [pairs[c, pl.ds(k, samples, stride=mixes), :] for c in range(features // 128)], axis=1
        ).astype(jnp.bfloat16)
        total = total + jnp.dot(lhs, weight_vmem[k], preferred_element_type=jnp.float32)
    out_ref[...] = jnp.maximum(total, 0.0).astype(jnp.bfloat16)


def score_samples(base, selectors, arrived, compress, weight, bias, most_rows):
    mixes, features = compress.shape
    units = weight.shape[2]
    groups, _, emb = arrived[0].shape
    samples = 2 * selectors.shape[1] // BLOCK
    vmem = pl.BlockSpec(memory_space=pltpu.VMEM)
    hbm = pl.BlockSpec(memory_space=pltpu.HBM)
    return pl.pallas_call(
        functools.partial(tail_kernel, most_rows=most_rows),
        out_shape=jax.ShapeDtypeStruct((samples, units), jnp.bfloat16),
        in_specs=[pl.BlockSpec(memory_space=pltpu.SMEM), hbm, vmem, hbm, vmem]
        + [vmem] * len(arrived),
        out_specs=vmem,
        scratch_shapes=[
            pltpu.VMEM((groups * PACK_ROOM + most_rows, emb), jnp.float32),
            pltpu.VMEM((samples // 2, 2, features, emb), jnp.bfloat16),
            pltpu.VMEM((features // 128, samples * mixes, 128), jnp.float32),
            pltpu.VMEM((4, 2 * emb, features), jnp.bfloat16),
            pltpu.VMEM(selectors.shape, jnp.bfloat16),
            pltpu.VMEM(weight.shape, jnp.bfloat16),
            pltpu.SemaphoreType.DMA((PARTS,)),
            pltpu.SemaphoreType.DMA(()),
        ],
        compiler_params=pltpu.CompilerParams(vmem_limit_bytes=53 << 20),
        cost_estimate=pl.CostEstimate(flops=20_000_000_000, bytes_accessed=16 << 20, transcendentals=0),
    )(base, selectors, compress, weight, bias, *arrived)


def shards(
    tables, bag_rows, bag_lengths, row_counts, inverse, table_order, compress, top_weight, top_bias
):
    vocabulary, emb = tables.shape[1:]
    slots = table_order.shape[0]
    most_rows = bag_rows.shape[2]
    mixes = compress.shape[0]
    counts = row_counts[0]
    message = bag_message(bag_rows[0], bag_lengths[0], row_counts, vocabulary)
    got = lax.all_to_all(message, "dev", split_axis=0, concat_axis=0, tiled=True)
    table_rows = tables.reshape(-1, emb)
    arrived = []
    for first, count in CHUNKS:
        pooled = pool_rows(got, table_rows, first, count)
        arrived.append(lax.all_to_all(pooled, "dev", split_axis=0, concat_axis=0, tiled=True))

    grouped = counts.reshape(-1, GROUP)
    before = jnp.cumsum(grouped, axis=1) - grouped
    group_at = jnp.arange(slots // GROUP, dtype=jnp.int32)[:, None] * PACK_ROOM
    slot_base = (before + group_at).reshape(-1)
    slot_range = jnp.arange(slots, dtype=jnp.int32)
    matches = table_order[:, None] == slot_range[None, :]
    feature_base = jnp.sum(jnp.where(matches, slot_base[:, None], 0), axis=0)
    feature_count = jnp.sum(jnp.where(matches, counts[:, None], 0), axis=0)
    shift = (slot_range % (BLOCK // 2)) * most_rows
    pos = jnp.where(inverse < feature_count[None, :], inverse + shift[None, :], -1)
    selectors = build_selectors(jnp.transpose(pos.astype(jnp.float32), (1, 0)))
    weight = jnp.transpose(top_weight.reshape(slots, mixes, -1), (1, 0, 2))
    return score_samples(
        feature_base, selectors, arrived, compress, weight, top_bias[None, :], most_rows
    )


def solution(mesh):
    return jax.shard_map(
        shards,
        mesh=mesh,
        in_specs=(
            P("dev", None, None),
            P(("rep", "dev"), None, None, None),
            P(("rep", "dev"), None, None),
            P(("rep", "dev"), None),
            P(("rep", "dev"), None),
            P(),
            P(),
            P(),
            P(),
        ),
        out_specs=P(("rep", "dev"), None),
        check_vma=False,
    )
```

```python
import functools

import jax
import jax.numpy as jnp
from jax import lax
from jax.experimental import pallas as pl
from jax.experimental.pallas import tpu as pltpu
from jax.sharding import PartitionSpec as P

PACK_ROOM = 80
CHUNKS = ((0, 80),)
BLOCK = 8
PARTS = 8
SENDERS = 2
GROUP = 4


def message_kernel(ids_ref, lengths_ref, counts_ref, out_ref, words, *, vocabulary):
    most_rows, pool, slots = ids_ref.shape
    spare = GROUP * vocabulary
    slot = lax.broadcasted_iota(jnp.int32, (8, slots), 1) % GROUP
    counts = jnp.broadcast_to(counts_ref[...], (8, slots))
    offset = jnp.zeros((8, slots), jnp.int32)
    for back in range(1, GROUP):
        offset = offset + jnp.where(slot >= back, pltpu.roll(counts, back, 1), 0)
    offset = offset[:1, :]
    table = slot[:1, :] * vocabulary
    lengths = lengths_ref[...]
    used = lax.broadcasted_iota(jnp.int32, (most_rows, slots), 0) < counts[:1, :]
    room = 128
    for h in range(pool // 2):
        low = jnp.where(2 * h < lengths, ids_ref[:, 2 * h, :] + table, spare)
        high = jnp.where(2 * h + 1 < lengths, ids_ref[:, 2 * h + 1, :] + table, spare)
        word = jnp.where(used, low | (high << 16), 0)
        word = jnp.concatenate([word, jnp.zeros((8, slots), jnp.int32)], axis=0)
        for bit in range(3):
            moved = pltpu.roll(word, 1 << bit, 0)
            word = jnp.where(((offset >> bit) & 1) == 1, moved, word)
        word = jnp.concatenate(
            [word, jnp.zeros((room - word.shape[0], slots), jnp.int32)], axis=0
        )
        for bit in range(3, 7):
            by = 1 << bit
            moved = jnp.concatenate(
                [jnp.zeros((by, slots), jnp.int32), word[: room - by, :]], axis=0
            )
            word = jnp.where(((offset >> bit) & 1) == 1, moved, word)
        words[...] = jnp.transpose(word, (1, 0))
        groups = slots // GROUP
        total = words[pl.ds(0, groups, stride=GROUP), :]
        for member in range(1, GROUP):
            total = total + words[pl.ds(member, groups, stride=GROUP), :]
        out_ref[pl.ds(h, groups, stride=pool // 2), :] = total


def bag_message(bag_rows, bag_lengths, counts, vocabulary):
    slots, most_rows, pool = bag_rows.shape
    groups = slots // GROUP
    message = pl.pallas_call(
        functools.partial(message_kernel, vocabulary=vocabulary),
        out_shape=jax.ShapeDtypeStruct((groups * pool // 2, 128), jnp.int32),
        in_specs=[pl.BlockSpec(memory_space=pltpu.VMEM)] * 3,
        out_specs=pl.BlockSpec(memory_space=pltpu.VMEM),
        scratch_shapes=[pltpu.VMEM((slots, 128), jnp.int32)],
    )(jnp.transpose(bag_rows, (1, 2, 0)), jnp.transpose(bag_lengths, (1, 0)), counts)
    return message.reshape(groups, pool // 2, 128)


def pool_kernel(
    msg_ref, table_hbm, out_ref, table_ref, table_f32, pooled, ids, ids_smem, sems, table_sem,
    *, first, rows, pool,
):
    vocab_rows, emb = table_hbm.shape
    table_copy = pltpu.make_async_copy(table_hbm, table_ref, table_sem)
    table_copy.start()
    peers = out_ref.shape[0]
    lanes = ids.shape[1]
    per = min(pool, lanes // rows)
    lines = -(-pool // per)
    shares = sems.shape[0]
    lane = lax.broadcasted_iota(jnp.int32, (peers, lanes), 1)
    held = []
    for h in range(pool // 2):
        word = msg_ref[pl.ds(h, peers, stride=pool // 2), :]
        held += [word & 0xFFFF, lax.shift_right_logical(word, 16)]
    for q in range(lines):
        line = jnp.zeros((peers, lanes), jnp.int32)
        for r in range(per):
            moved = pltpu.roll(held[q * per + r], (r * rows - first) % lanes, 1)
            line = jnp.where((lane >= r * rows) & (lane < (r + 1) * rows), moved, line)
        ids[pl.ds(q, peers, stride=lines), :] = line
    step = peers // shares
    copies = [
        pltpu.make_async_copy(
            ids.at[pl.ds(c * step * lines, step * lines)],
            ids_smem.at[pl.ds(c * step * lines, step * lines)],
            sems.at[c],
        )
        for c in range(shares)
    ]
    for copy in copies:
        copy.start()
    table_f32[pl.ds(vocab_rows, 8), :] = jnp.zeros((8, emb), jnp.float32)
    table_copy.wait()

    def widen(i, carry):
        at = pl.multiple_of(i * 256, 256)
        table_f32[pl.ds(at, 256), :] = table_ref[pl.ds(at, 256), :].astype(jnp.float32)
        return carry

    lax.fori_loop(0, vocab_rows // 256, widen, 0)

    def some_senders(i, carry):
        views = [
            [ids_smem.at[pl.ds((i * SENDERS + n) * lines + q, 1)] for q in range(lines)]
            for n in range(SENDERS)
        ]
        for j in range(rows):
            for n in range(SENDERS):
                parts = [
                    table_f32[pl.ds(views[n][p // per][0, (p % per) * rows + j], 1), :]
                    for p in range(pool)
                ]
                while len(parts) > 1:
                    parts = [parts[m] + parts[m + 1] for m in range(0, len(parts), 2)]
                pooled[pl.ds((i * SENDERS + n) * rows + j, 1), :] = parts[0]
        return carry

    for c in range(shares):
        copies[c].wait()
        lax.fori_loop(c * step // SENDERS, (c + 1) * step // SENDERS, some_senders, 0)

    def narrow(d, carry):
        at = pl.multiple_of(d * rows, 8)
        out_ref[d] = pooled[pl.ds(at, rows), :].astype(jnp.bfloat16)
        return carry

    lax.fori_loop(0, peers, narrow, 0, unroll=4)


def pool_rows(message, table_rows, first, rows):
    peers, halves, width = message.shape
    pool = 2 * halves
    lines = -(-pool // min(pool, width // rows))
    emb = table_rows.shape[1]
    vmem = pl.BlockSpec(memory_space=pltpu.VMEM)
    return pl.pallas_call(
        functools.partial(pool_kernel, first=first, rows=rows, pool=pool),
        out_shape=jax.ShapeDtypeStruct((peers, rows, emb), jnp.bfloat16),
        in_specs=[vmem, pl.BlockSpec(memory_space=pltpu.HBM)],
        out_specs=vmem,
        scratch_shapes=[
            pltpu.VMEM(table_rows.shape, jnp.bfloat16),
            pltpu.VMEM((table_rows.shape[0] + 8, emb), jnp.float32),
            pltpu.VMEM((peers * rows, emb), jnp.float32),
            pltpu.VMEM((peers * lines, width), jnp.int32),
            pltpu.SMEM((peers * lines, width), jnp.int32),
            pltpu.SemaphoreType.DMA((4,)),
            pltpu.SemaphoreType.DMA(()),
        ],
        compiler_params=pltpu.CompilerParams(vmem_limit_bytes=125 << 19),
        cost_estimate=pl.CostEstimate(flops=20_000_000_000, bytes_accessed=5 << 20, transcendentals=0),
    )(message.reshape(peers * halves, width), table_rows)


def selector_kernel(pos_ref, out_ref):
    blocks, rows, lanes = out_ref.shape
    pairs = rows // BLOCK
    half = lanes // 2
    lane = lax.broadcasted_iota(jnp.int32, (BLOCK, half), 1).astype(jnp.float32)
    upper = lax.broadcasted_iota(jnp.int32, (BLOCK, pos_ref.shape[1]), 0) < BLOCK // 2

    def one_block(i, carry):
        here = pos_ref[pl.ds(pl.multiple_of(i * BLOCK, BLOCK), BLOCK), :]
        swapped = pltpu.roll(here, BLOCK // 2, 0)
        samples = here.shape[1]
        sides = (
            jnp.where(upper, here, pltpu.roll(swapped, samples - 1, 1)),
            jnp.where(upper, swapped, pltpu.roll(here, samples - 1, 1)),
        )
        for side, pos in enumerate(sides):
            for p in range(0, pairs, 2):
                both = [
                    jnp.where(jnp.broadcast_to(pos[:, c : c + 1], (BLOCK, half)) == lane, 1.0, 0.0)
                    for c in (2 * p, 2 * p + 2)
                ]
                out_ref[i, pl.ds(p * BLOCK, 2 * BLOCK), pl.ds(side * half, half)] = (
                    jnp.concatenate(both, axis=0).astype(jnp.bfloat16)
                )
        return carry

    lax.fori_loop(0, blocks, one_block, 0)


def build_selectors(pos):
    features, samples = pos.shape
    blocks = features // BLOCK
    pairs = samples // 2
    some = 4
    return pl.pallas_call(
        selector_kernel,
        grid=(blocks // some,),
        out_shape=jax.ShapeDtypeStruct((blocks, pairs * BLOCK, 256), jnp.bfloat16),
        in_specs=[pl.BlockSpec((some * BLOCK, samples), lambda i: (i, 0))],
        out_specs=pl.BlockSpec((some, pairs * BLOCK, 256), lambda i: (i, 0, 0)),
        compiler_params=pltpu.CompilerParams(vmem_limit_bytes=8 << 20),
        cost_estimate=pl.CostEstimate(flops=10_000_000_000, bytes_accessed=16 << 20, transcendentals=0),
    )(pos)


def tail_kernel(base_ref, selector_ref, compress_ref, weight_ref, bias_ref, *refs, most_rows):
    row_refs = refs[: len(CHUNKS)]
    (
        out_ref, rows_f32, feats, pairs, turned, select_vmem, weight_vmem, select_sem, weight_sem,
    ) = refs[len(CHUNKS) :]
    groups, _, emb = row_refs[0].shape
    total_rows = groups * PACK_ROOM
    sample_pairs, _, features, _ = feats.shape
    samples = 2 * sample_pairs
    mixes = compress_ref.shape[0]
    blocks = features // BLOCK
    share = blocks // PARTS
    copies = [
        pltpu.make_async_copy(
            selector_ref.at[pl.ds(part * share, share)],
            select_vmem.at[pl.ds(part * share, share)],
            select_sem.at[part],
        )
        for part in range(PARTS)
    ]
    for copy in copies:
        copy.start()
    weight_copy = pltpu.make_async_copy(weight_ref, weight_vmem, weight_sem)
    weight_copy.start()

    rows_f32[pl.ds(total_rows, most_rows), :] = jnp.zeros((most_rows, emb), jnp.float32)

    def widen(g, carry):
        for (first, count), row_ref in zip(CHUNKS, row_refs):
            at = pl.multiple_of(g * PACK_ROOM + first, 16)
            rows_f32[pl.ds(at, count), :] = row_ref[g].astype(jnp.float32)
        return carry

    lax.fori_loop(0, groups, widen, 0, unroll=4)

    first_half = lax.broadcasted_iota(jnp.int32, (1, BLOCK, emb), 1) < BLOCK // 2
    some = 32
    empty = jnp.zeros((BLOCK // 2 * most_rows, emb), jnp.bfloat16)

    def expand(i, carry):
        for pair in range(2):
            tops = []
            for half in range(2):
                block = 4 * i + 2 * pair + half
                sides = []
                for side in range(2):
                    parts = []
                    for j in range(BLOCK // 2):
                        base = base_ref[block * BLOCK + side * (BLOCK // 2) + j]
                        parts.append(rows_f32[pl.ds(base, most_rows), :].astype(jnp.bfloat16))
                    sides.append(jnp.concatenate(parts, axis=0))
                top = jnp.concatenate([sides[0], empty], axis=1)
                bottom = jnp.concatenate([empty, sides[1]], axis=1)
                tops.append((block, jnp.concatenate([top, bottom], axis=0)))
            at = pl.multiple_of((4 * i + 2 * pair) * BLOCK, 2 * BLOCK)
            for c in range(sample_pairs // some):
                even, odd = [], []
                for block, rhs in tops:
                    lhs = select_vmem[block, pl.ds(c * some * BLOCK, some * BLOCK), :]
                    got = jnp.dot(lhs, rhs, preferred_element_type=jnp.float32)
                    got = got.reshape(some, BLOCK, 2 * emb)
                    left, right = got[:, :, :emb], got[:, :, emb:]
                    even.append(jnp.where(first_half, left, pltpu.roll(right, BLOCK // 2, 1)))
                    odd.append(jnp.where(first_half, pltpu.roll(left, BLOCK // 2, 1), right))
                for which, parts in enumerate((even, odd)):
                    feats[pl.ds(c * some, some), which, pl.ds(at, 2 * BLOCK), :] = jnp.concatenate(
                        parts, axis=1
                    ).astype(jnp.bfloat16)
        return carry

    for part in range(PARTS):
        copies[part].wait()
        lax.fori_loop(part * share // 4, (part + 1) * share // 4, expand, 0)

    per = 8

    def score(i, carry):
        mixing = compress_ref[...]
        mixed = []
        for j in range(per // 2):
            at = i * (per // 2) + j
            both = jnp.concatenate([feats[at, 0], feats[at, 1]], axis=1)
            turned[j] = jnp.transpose(both)
            mixed.append(
                jnp.dot(mixing, both, preferred_element_type=jnp.float32).astype(jnp.bfloat16)
            )
        for j in range(per // 2):
            none = jnp.zeros((mixes, emb), jnp.bfloat16)
            first = jnp.concatenate([mixed[j][:, :emb], none], axis=1)
            second = jnp.concatenate([none, mixed[j][:, emb:]], axis=1)
            lhs = jnp.concatenate([first, second], axis=0)
            got = jnp.dot(lhs, turned[j], preferred_element_type=jnp.float32)
            at = pl.multiple_of((i * per + 2 * j) * mixes, 2 * mixes)
            for c in range(features // 128):
                pairs[c, pl.ds(at, 2 * mixes), :] = got[:, c * 128 : (c + 1) * 128]
        return carry

    lax.fori_loop(0, samples // per, score, 0)

    weight_copy.wait()
    total = jnp.broadcast_to(bias_ref[...], (samples, out_ref.shape[1]))
    for k in range(mixes):
        lhs = jnp.concatenate(
            [pairs[c, pl.ds(k, samples, stride=mixes), :] for c in range(features // 128)], axis=1
        ).astype(jnp.bfloat16)
        total = total + jnp.dot(lhs, weight_vmem[k], preferred_element_type=jnp.float32)
    out_ref[...] = jnp.maximum(total, 0.0).astype(jnp.bfloat16)


def score_samples(base, selectors, arrived, compress, weight, bias, most_rows):
    mixes, features = compress.shape
    units = weight.shape[2]
    groups, _, emb = arrived[0].shape
    samples = 2 * selectors.shape[1] // BLOCK
    vmem = pl.BlockSpec(memory_space=pltpu.VMEM)
    hbm = pl.BlockSpec(memory_space=pltpu.HBM)
    return pl.pallas_call(
        functools.partial(tail_kernel, most_rows=most_rows),
        out_shape=jax.ShapeDtypeStruct((samples, units), jnp.bfloat16),
        in_specs=[pl.BlockSpec(memory_space=pltpu.SMEM), hbm, vmem, hbm, vmem]
        + [vmem] * len(arrived),
        out_specs=vmem,
        scratch_shapes=[
            pltpu.VMEM((groups * PACK_ROOM + most_rows, emb), jnp.float32),
            pltpu.VMEM((samples // 2, 2, features, emb), jnp.bfloat16),
            pltpu.VMEM((features // 128, samples * mixes, 128), jnp.float32),
            pltpu.VMEM((4, 2 * emb, features), jnp.bfloat16),
            pltpu.VMEM(selectors.shape, jnp.bfloat16),
            pltpu.VMEM(weight.shape, jnp.bfloat16),
            pltpu.SemaphoreType.DMA((PARTS,)),
            pltpu.SemaphoreType.DMA(()),
        ],
        compiler_params=pltpu.CompilerParams(vmem_limit_bytes=125 << 19),
        cost_estimate=pl.CostEstimate(flops=20_000_000_000, bytes_accessed=16 << 20, transcendentals=0),
    )(base, selectors, compress, weight, bias, *arrived)


def shards(
    tables, bag_rows, bag_lengths, row_counts, inverse, table_order, compress, top_weight, top_bias
):
    vocabulary, emb = tables.shape[1:]
    slots = table_order.shape[0]
    most_rows = bag_rows.shape[2]
    mixes = compress.shape[0]
    counts = row_counts[0]
    message = bag_message(bag_rows[0], bag_lengths[0], row_counts, vocabulary)
    got = lax.all_to_all(message, "dev", split_axis=0, concat_axis=0, tiled=True)
    table_rows = tables.reshape(-1, emb)
    arrived = []
    for first, count in CHUNKS:
        pooled = pool_rows(got, table_rows, first, count)
        arrived.append(lax.all_to_all(pooled, "dev", split_axis=0, concat_axis=0, tiled=True))

    grouped = counts.reshape(-1, GROUP)
    before = jnp.cumsum(grouped, axis=1) - grouped
    group_at = jnp.arange(slots // GROUP, dtype=jnp.int32)[:, None] * PACK_ROOM
    slot_base = (before + group_at).reshape(-1)
    slot_range = jnp.arange(slots, dtype=jnp.int32)
    matches = table_order[:, None] == slot_range[None, :]
    feature_base = jnp.sum(jnp.where(matches, slot_base[:, None], 0), axis=0)
    feature_count = jnp.sum(jnp.where(matches, counts[:, None], 0), axis=0)
    shift = (slot_range % (BLOCK // 2)) * most_rows
    pos = jnp.where(inverse < feature_count[None, :], inverse + shift[None, :], -1)
    selectors = build_selectors(jnp.transpose(pos.astype(jnp.float32), (1, 0)))
    weight = jnp.transpose(top_weight.reshape(slots, mixes, -1), (1, 0, 2))
    return score_samples(
        feature_base, selectors, arrived, compress, weight, top_bias[None, :], most_rows
    )


def solution(mesh):
    return jax.shard_map(
        shards,
        mesh=mesh,
        in_specs=(
            P("dev", None, None),
            P(("rep", "dev"), None, None, None),
            P(("rep", "dev"), None, None),
            P(("rep", "dev"), None),
            P(("rep", "dev"), None),
            P(),
            P(),
            P(),
            P(),
        ),
        out_specs=P(("rep", "dev"), None),
        check_vma=False,
    )
```

```python
import functools

import jax
import jax.numpy as jnp
from jax import lax
from jax.experimental import pallas as pl
from jax.experimental.pallas import tpu as pltpu
from jax.sharding import PartitionSpec as P

PACK_ROOM = 80
BLOCK = 8
PARTS = 8
AHEAD = 3
WEIGHTS_AT = 5
SENDERS = 2
SHARES = 8
GROUP = 4


def message_kernel(ids_ref, lengths_ref, counts_ref, out_ref, words, *, vocabulary):
    most_rows, pool, slots = ids_ref.shape
    spare = GROUP * vocabulary
    slot = lax.broadcasted_iota(jnp.int32, (8, slots), 1) % GROUP
    counts = jnp.broadcast_to(counts_ref[...], (8, slots))
    offset = jnp.zeros((8, slots), jnp.int32)
    for back in range(1, GROUP):
        offset = offset + jnp.where(slot >= back, pltpu.roll(counts, back, 1), 0)
    offset = offset[:1, :]
    table = slot[:1, :] * vocabulary
    lengths = lengths_ref[...]
    used = lax.broadcasted_iota(jnp.int32, (most_rows, slots), 0) < counts[:1, :]
    room = 128
    for h in range(pool // 2):
        low = jnp.where(2 * h < lengths, ids_ref[:, 2 * h, :] + table, spare)
        high = jnp.where(2 * h + 1 < lengths, ids_ref[:, 2 * h + 1, :] + table, spare)
        word = jnp.where(used, low | (high << 16), 0)
        word = jnp.concatenate([word, jnp.zeros((8, slots), jnp.int32)], axis=0)
        for bit in range(3):
            moved = pltpu.roll(word, 1 << bit, 0)
            word = jnp.where(((offset >> bit) & 1) == 1, moved, word)
        word = jnp.concatenate(
            [word, jnp.zeros((room - word.shape[0], slots), jnp.int32)], axis=0
        )
        for bit in range(3, 7):
            by = 1 << bit
            moved = jnp.concatenate(
                [jnp.zeros((by, slots), jnp.int32), word[: room - by, :]], axis=0
            )
            word = jnp.where(((offset >> bit) & 1) == 1, moved, word)
        words[...] = jnp.transpose(word, (1, 0))
        groups = slots // GROUP
        total = words[pl.ds(0, groups, stride=GROUP), :]
        for member in range(1, GROUP):
            total = total + words[pl.ds(member, groups, stride=GROUP), :]
        out_ref[pl.ds(h, groups, stride=pool // 2), :] = total


def bag_message(bag_rows, bag_lengths, counts, vocabulary):
    slots, most_rows, pool = bag_rows.shape
    groups = slots // GROUP
    message = pl.pallas_call(
        functools.partial(message_kernel, vocabulary=vocabulary),
        out_shape=jax.ShapeDtypeStruct((groups * pool // 2, 128), jnp.int32),
        in_specs=[pl.BlockSpec(memory_space=pltpu.VMEM)] * 3,
        out_specs=pl.BlockSpec(memory_space=pltpu.VMEM),
        scratch_shapes=[pltpu.VMEM((slots, 128), jnp.int32)],
    )(jnp.transpose(bag_rows, (1, 2, 0)), jnp.transpose(bag_lengths, (1, 0)), counts)
    return message.reshape(groups, pool // 2, 128)


def pool_kernel(
    msg_ref, table_hbm, out_hbm, table_ref, table_f32, pooled, out_ref, ids, ids_smem, sems,
    out_sems, table_sem,
    *, first, rows, pool,
):
    vocab_rows, emb = table_hbm.shape
    table_copy = pltpu.make_async_copy(table_hbm, table_ref, table_sem)
    table_copy.start()
    peers = out_ref.shape[0]
    lanes = ids.shape[1]
    per = min(pool, lanes // rows)
    lines = -(-pool // per)
    shares = sems.shape[0]
    lane = lax.broadcasted_iota(jnp.int32, (peers, lanes), 1)
    held = []
    for h in range(pool // 2):
        word = msg_ref[pl.ds(h, peers, stride=pool // 2), :]
        held += [word & 0xFFFF, lax.shift_right_logical(word, 16)]
    for q in range(lines):
        line = jnp.zeros((peers, lanes), jnp.int32)
        for r in range(per):
            moved = pltpu.roll(held[q * per + r], (r * rows - first) % lanes, 1)
            line = jnp.where((lane >= r * rows) & (lane < (r + 1) * rows), moved, line)
        ids[pl.ds(q, peers, stride=lines), :] = line
    step = peers // shares
    copies = [
        pltpu.make_async_copy(
            ids.at[pl.ds(c * step * lines, step * lines)],
            ids_smem.at[pl.ds(c * step * lines, step * lines)],
            sems.at[c],
        )
        for c in range(shares)
    ]
    for copy in copies:
        copy.start()
    table_f32[pl.ds(vocab_rows, 8), :] = jnp.zeros((8, emb), jnp.float32)
    table_copy.wait()

    def widen(i, carry):
        at = pl.multiple_of(i * 256, 256)
        table_f32[pl.ds(at, 256), :] = table_ref[pl.ds(at, 256), :].astype(jnp.float32)
        return carry

    lax.fori_loop(0, vocab_rows // 256, widen, 0)

    def some_senders(i, carry):
        views = [
            [ids_smem.at[pl.ds((i * SENDERS + n) * lines + q, 1)] for q in range(lines)]
            for n in range(SENDERS)
        ]
        for j in range(rows):
            for n in range(SENDERS):
                parts = [
                    table_f32[pl.ds(views[n][p // per][0, (p % per) * rows + j], 1), :]
                    for p in range(pool)
                ]
                while len(parts) > 1:
                    parts = [parts[m] + parts[m + 1] for m in range(0, len(parts), 2)]
                pooled[pl.ds((i * SENDERS + n) * rows + j, 1), :] = parts[0]
        return carry

    def narrow(d, carry):
        at = pl.multiple_of(d * rows, 8)
        out_ref[d] = pooled[pl.ds(at, rows), :].astype(jnp.bfloat16)
        return carry

    outs = [
        pltpu.make_async_copy(
            out_ref.at[pl.ds(c * step, step)], out_hbm.at[pl.ds(c * step, step)], out_sems.at[c]
        )
        for c in range(shares)
    ]
    for c in range(shares):
        copies[c].wait()
        lax.fori_loop(c * step // SENDERS, (c + 1) * step // SENDERS, some_senders, 0)
        lax.fori_loop(c * step, (c + 1) * step, narrow, 0, unroll=4)
        outs[c].start()
    for c in range(shares):
        outs[c].wait()


def pool_rows(message, table_rows, first, rows):
    peers, halves, width = message.shape
    pool = 2 * halves
    lines = -(-pool // min(pool, width // rows))
    emb = table_rows.shape[1]
    vmem = pl.BlockSpec(memory_space=pltpu.VMEM)
    return pl.pallas_call(
        functools.partial(pool_kernel, first=first, rows=rows, pool=pool),
        out_shape=jax.ShapeDtypeStruct((peers, rows, emb), jnp.bfloat16),
        in_specs=[vmem, pl.BlockSpec(memory_space=pltpu.HBM)],
        out_specs=pl.BlockSpec(memory_space=pltpu.HBM),
        scratch_shapes=[
            pltpu.VMEM(table_rows.shape, jnp.bfloat16),
            pltpu.VMEM((table_rows.shape[0] + 8, emb), jnp.float32),
            pltpu.VMEM((peers * rows, emb), jnp.float32),
            pltpu.VMEM((peers, rows, emb), jnp.bfloat16),
            pltpu.VMEM((peers * lines, width), jnp.int32),
            pltpu.SMEM((peers * lines, width), jnp.int32),
            pltpu.SemaphoreType.DMA((SHARES,)),
            pltpu.SemaphoreType.DMA((SHARES,)),
            pltpu.SemaphoreType.DMA(()),
        ],
        compiler_params=pltpu.CompilerParams(vmem_limit_bytes=125 << 19),
        cost_estimate=pl.CostEstimate(flops=20_000_000_000, bytes_accessed=5 << 20, transcendentals=0),
    )(message.reshape(peers * halves, width), table_rows)


def selector_kernel(pos_ref, out_ref):
    blocks, rows, lanes = out_ref.shape
    pairs = rows // BLOCK
    half = lanes
    lane = lax.broadcasted_iota(jnp.int32, (BLOCK, half), 1).astype(jnp.float32)
    upper = lax.broadcasted_iota(jnp.int32, (BLOCK, pos_ref.shape[1]), 0) < BLOCK // 2

    def one_block(i, carry):
        here = pos_ref[pl.ds(pl.multiple_of(i * BLOCK, BLOCK), BLOCK), :]
        swapped = pltpu.roll(here, BLOCK // 2, 0)
        samples = here.shape[1]
        sides = (
            jnp.where(upper, here, pltpu.roll(swapped, samples - 1, 1)),
            jnp.where(upper, swapped, pltpu.roll(here, samples - 1, 1)),
        )
        for p in range(0, pairs, 2):
            both = []
            for c in (2 * p, 2 * p + 2):
                marks = [
                    jnp.where(jnp.broadcast_to(pos[:, c : c + 1], (BLOCK, half)) == lane, mark, 0.0)
                    for mark, pos in zip((1.0, 2.0), sides)
                ]
                both.append(marks[0] + marks[1])
            out_ref[i, pl.ds(p * BLOCK, 2 * BLOCK), :] = jnp.concatenate(both, axis=0).astype(
                jnp.bfloat16
            )
        return carry

    lax.fori_loop(0, blocks, one_block, 0)


def build_selectors(pos):
    features, samples = pos.shape
    blocks = features // BLOCK
    pairs = samples // 2
    some = 4
    return pl.pallas_call(
        selector_kernel,
        grid=(blocks // some,),
        out_shape=jax.ShapeDtypeStruct((blocks, pairs * BLOCK, 128), jnp.bfloat16),
        in_specs=[pl.BlockSpec((some * BLOCK, samples), lambda i: (i, 0))],
        out_specs=pl.BlockSpec((some, pairs * BLOCK, 128), lambda i: (i, 0, 0)),
        compiler_params=pltpu.CompilerParams(vmem_limit_bytes=8 << 20),
        cost_estimate=pl.CostEstimate(flops=10_000_000_000, bytes_accessed=8 << 20, transcendentals=0),
    )(pos)


def tail_kernel(
    base_ref, selector_ref, compress_ref, weight_ref, bias_ref, arrived_ref, out_ref,
    rows_bf16, rows_f32, feats, pairs, turned, select_vmem, weight_vmem,
    row_sem, select_sem, weight_sem, *, most_rows,
):
    groups, _, emb = arrived_ref.shape
    total_rows = groups * PACK_ROOM
    sample_pairs, _, features, _ = feats.shape
    samples = 2 * sample_pairs
    mixes = compress_ref.shape[0]
    blocks = features // BLOCK
    share = blocks // PARTS
    quarter = groups // 4
    row_copies = [
        pltpu.make_async_copy(
            arrived_ref.at[pl.ds(c * quarter, quarter)],
            rows_bf16.at[pl.ds(c * quarter, quarter)],
            row_sem.at[c],
        )
        for c in range(4)
    ]
    copies = [
        pltpu.make_async_copy(
            selector_ref.at[pl.ds(part * share, share)],
            select_vmem.at[pl.ds(part * share, share)],
            select_sem.at[part],
        )
        for part in range(PARTS)
    ]
    weight_copy = pltpu.make_async_copy(weight_ref, weight_vmem, weight_sem)
    for copy in row_copies + copies[:1]:
        copy.start()

    rows_f32[pl.ds(total_rows, most_rows), :] = jnp.zeros((most_rows, emb), jnp.float32)

    def widen(g, carry):
        at = pl.multiple_of(g * PACK_ROOM, 16)
        rows_f32[pl.ds(at, PACK_ROOM), :] = rows_bf16[g].astype(jnp.float32)
        return carry

    for c in range(4):
        row_copies[c].wait()
        lax.fori_loop(c * quarter, (c + 1) * quarter, widen, 0, unroll=4)
    for copy in copies[1:AHEAD]:
        copy.start()

    first_half = lax.broadcasted_iota(jnp.int32, (1, BLOCK, emb), 1) < BLOCK // 2
    some = 32
    empty = jnp.zeros((BLOCK // 2 * most_rows, emb), jnp.bfloat16)
    zero = jnp.zeros((some * BLOCK, BLOCK // 2 * most_rows), jnp.bfloat16)
    one = jnp.ones_like(zero)
    two = one + one

    def expand(i, carry):
        for pair in range(2):
            tops = []
            for half in range(2):
                block = 4 * i + 2 * pair + half
                sides = []
                for side in range(2):
                    parts = []
                    for j in range(BLOCK // 2):
                        base = base_ref[block * BLOCK + side * (BLOCK // 2) + j]
                        parts.append(rows_f32[pl.ds(base, most_rows), :].astype(jnp.bfloat16))
                    sides.append(jnp.concatenate(parts, axis=0))
                top = jnp.concatenate([sides[0], empty], axis=1)
                bottom = jnp.concatenate([empty, sides[1]], axis=1)
                tops.append((block, jnp.concatenate([top, bottom], axis=0)))
            at = pl.multiple_of((4 * i + 2 * pair) * BLOCK, 2 * BLOCK)
            for c in range(sample_pairs // some):
                even, odd = [], []
                for block, rhs in tops:
                    marks = select_vmem[block, pl.ds(c * some * BLOCK, some * BLOCK), :]
                    second = jnp.where(marks >= two, one, zero)
                    lhs = jnp.concatenate([marks - second - second, second], axis=1)
                    got = jnp.dot(lhs, rhs, preferred_element_type=jnp.float32)
                    got = got.reshape(some, BLOCK, 2 * emb)
                    left, right = got[:, :, :emb], got[:, :, emb:]
                    even.append(jnp.where(first_half, left, pltpu.roll(right, BLOCK // 2, 1)))
                    odd.append(jnp.where(first_half, pltpu.roll(left, BLOCK // 2, 1), right))
                for which, parts in enumerate((even, odd)):
                    feats[pl.ds(c * some, some), which, pl.ds(at, 2 * BLOCK), :] = jnp.concatenate(
                        parts, axis=1
                    ).astype(jnp.bfloat16)
        return carry

    for part in range(PARTS):
        copies[part].wait()
        if part + AHEAD < PARTS:
            copies[part + AHEAD].start()
        if part == WEIGHTS_AT:
            weight_copy.start()
        lax.fori_loop(part * share // 4, (part + 1) * share // 4, expand, 0)

    per = 8

    def score(i, carry):
        mixing = compress_ref[...]
        mixed = []
        for j in range(per // 2):
            at = i * (per // 2) + j
            both = jnp.concatenate([feats[at, 0], feats[at, 1]], axis=1)
            turned[j] = jnp.transpose(both)
            mixed.append(
                jnp.dot(mixing, both, preferred_element_type=jnp.float32).astype(jnp.bfloat16)
            )
        for j in range(per // 2):
            none = jnp.zeros((mixes, emb), jnp.bfloat16)
            first = jnp.concatenate([mixed[j][:, :emb], none], axis=1)
            second = jnp.concatenate([none, mixed[j][:, emb:]], axis=1)
            lhs = jnp.concatenate([first, second], axis=0)
            got = jnp.dot(lhs, turned[j], preferred_element_type=jnp.float32)
            for n in range(2 * mixes // BLOCK):
                sample = i * per + 2 * j + n * BLOCK // mixes
                at = pl.multiple_of(sample * BLOCK, BLOCK)
                for c in range(features // 128):
                    pairs[c, n % (mixes // BLOCK), pl.ds(at, BLOCK), :] = got[
                        n * BLOCK : (n + 1) * BLOCK, c * 128 : (c + 1) * 128
                    ]
        return carry

    lax.fori_loop(0, samples // per, score, 0)

    weight_copy.wait()
    total = jnp.broadcast_to(bias_ref[...], (samples, out_ref.shape[1]))
    for k in range(mixes):
        lhs = jnp.concatenate(
            [
                pairs[c, k // BLOCK, pl.ds(k % BLOCK, samples, stride=BLOCK), :]
                for c in range(features // 128)
            ],
            axis=1,
        ).astype(jnp.bfloat16)
        total = total + jnp.dot(lhs, weight_vmem[k], preferred_element_type=jnp.float32)
    out_ref[...] = jnp.maximum(total, 0.0).astype(jnp.bfloat16)


def score_samples(base, selectors, arrived, compress, weight, bias, most_rows):
    mixes, features = compress.shape
    units = weight.shape[2]
    groups, _, emb = arrived.shape
    samples = 2 * selectors.shape[1] // BLOCK
    vmem = pl.BlockSpec(memory_space=pltpu.VMEM)
    hbm = pl.BlockSpec(memory_space=pltpu.HBM)
    return pl.pallas_call(
        functools.partial(tail_kernel, most_rows=most_rows),
        out_shape=jax.ShapeDtypeStruct((samples, units), jnp.bfloat16),
        in_specs=[pl.BlockSpec(memory_space=pltpu.SMEM), hbm, vmem, hbm, vmem, hbm],
        out_specs=vmem,
        scratch_shapes=[
            pltpu.VMEM(arrived.shape, jnp.bfloat16),
            pltpu.VMEM((groups * PACK_ROOM + most_rows, emb), jnp.float32),
            pltpu.VMEM((samples // 2, 2, features, emb), jnp.bfloat16),
            pltpu.VMEM((features // 128, mixes // BLOCK, samples * BLOCK, 128), jnp.float32),
            pltpu.VMEM((4, 2 * emb, features), jnp.bfloat16),
            pltpu.VMEM(selectors.shape, jnp.bfloat16),
            pltpu.VMEM(weight.shape, jnp.bfloat16),
            pltpu.SemaphoreType.DMA((4,)),
            pltpu.SemaphoreType.DMA((PARTS,)),
            pltpu.SemaphoreType.DMA(()),
        ],
        compiler_params=pltpu.CompilerParams(vmem_limit_bytes=125 << 19),
        cost_estimate=pl.CostEstimate(flops=20_000_000_000, bytes_accessed=16 << 20, transcendentals=0),
    )(base, selectors, compress, weight, bias, arrived)


def shards(
    tables, bag_rows, bag_lengths, row_counts, inverse, table_order, compress, top_weight, top_bias
):
    vocabulary, emb = tables.shape[1:]
    slots = table_order.shape[0]
    most_rows = bag_rows.shape[2]
    mixes = compress.shape[0]
    counts = row_counts[0]
    message = bag_message(bag_rows[0], bag_lengths[0], row_counts, vocabulary)
    got = lax.all_to_all(message, "dev", split_axis=0, concat_axis=0, tiled=True)
    table_rows = tables.reshape(-1, emb)
    pooled = pool_rows(got, table_rows, 0, PACK_ROOM)
    arrived = lax.all_to_all(pooled, "dev", split_axis=0, concat_axis=0, tiled=True)

    grouped = counts.reshape(-1, GROUP)
    before = jnp.cumsum(grouped, axis=1) - grouped
    group_at = jnp.arange(slots // GROUP, dtype=jnp.int32)[:, None] * PACK_ROOM
    slot_base = (before + group_at).reshape(-1)
    slot_range = jnp.arange(slots, dtype=jnp.int32)
    matches = table_order[:, None] == slot_range[None, :]
    feature_base = jnp.sum(jnp.where(matches, slot_base[:, None], 0), axis=0)
    feature_count = jnp.sum(jnp.where(matches, counts[:, None], 0), axis=0)
    shift = (slot_range % (BLOCK // 2)) * most_rows
    pos = jnp.where(inverse < feature_count[None, :], inverse + shift[None, :], -1)
    selectors = build_selectors(jnp.transpose(pos.astype(jnp.float32), (1, 0)))
    weight = jnp.transpose(top_weight.reshape(slots, mixes, -1), (1, 0, 2))
    return score_samples(
        feature_base, selectors, arrived, compress, weight, top_bias[None, :], most_rows
    )


def solution(mesh):
    return jax.shard_map(
        shards,
        mesh=mesh,
        in_specs=(
            P("dev", None, None),
            P(("rep", "dev"), None, None, None),
            P(("rep", "dev"), None, None),
            P(("rep", "dev"), None),
            P(("rep", "dev"), None),
            P(),
            P(),
            P(),
            P(),
        ),
        out_specs=P(("rep", "dev"), None),
        check_vma=False,
    )
```

```python
import functools

import jax
import jax.numpy as jnp
from jax import lax
from jax.experimental import pallas as pl
from jax.experimental.pallas import tpu as pltpu
from jax.sharding import PartitionSpec as P

PACK_ROOM = 80
BLOCK = 8
PARTS = 8
AHEAD = 3
WEIGHTS_AT = 5
SENDERS = 2
SHARES = 8
GROUP = 4


def message_kernel(ids_ref, lengths_ref, counts_ref, out_ref, words, *, vocabulary):
    most_rows, pool, slots = ids_ref.shape
    spare = GROUP * vocabulary
    slot = lax.broadcasted_iota(jnp.int32, (8, slots), 1) % GROUP
    counts = jnp.broadcast_to(counts_ref[...], (8, slots))
    offset = jnp.zeros((8, slots), jnp.int32)
    for back in range(1, GROUP):
        offset = offset + jnp.where(slot >= back, pltpu.roll(counts, back, 1), 0)
    offset = offset[:1, :]
    table = slot[:1, :] * vocabulary
    lengths = lengths_ref[...]
    used = lax.broadcasted_iota(jnp.int32, (most_rows, slots), 0) < counts[:1, :]
    room = 128
    for h in range(pool // 2):
        low = jnp.where(2 * h < lengths, ids_ref[:, 2 * h, :] + table, spare)
        high = jnp.where(2 * h + 1 < lengths, ids_ref[:, 2 * h + 1, :] + table, spare)
        word = jnp.where(used, low | (high << 16), 0)
        word = jnp.concatenate([word, jnp.zeros((8, slots), jnp.int32)], axis=0)
        for bit in range(3):
            moved = pltpu.roll(word, 1 << bit, 0)
            word = jnp.where(((offset >> bit) & 1) == 1, moved, word)
        word = jnp.concatenate(
            [word, jnp.zeros((room - word.shape[0], slots), jnp.int32)], axis=0
        )
        for bit in range(3, 7):
            by = 1 << bit
            moved = jnp.concatenate(
                [jnp.zeros((by, slots), jnp.int32), word[: room - by, :]], axis=0
            )
            word = jnp.where(((offset >> bit) & 1) == 1, moved, word)
        words[...] = jnp.transpose(word, (1, 0))
        groups = slots // GROUP
        total = words[pl.ds(0, groups, stride=GROUP), :]
        for member in range(1, GROUP):
            total = total + words[pl.ds(member, groups, stride=GROUP), :]
        out_ref[pl.ds(h, groups, stride=pool // 2), :] = total


def bag_message(bag_rows, bag_lengths, counts, vocabulary):
    slots, most_rows, pool = bag_rows.shape
    groups = slots // GROUP
    message = pl.pallas_call(
        functools.partial(message_kernel, vocabulary=vocabulary),
        out_shape=jax.ShapeDtypeStruct((groups * pool // 2, 128), jnp.int32),
        in_specs=[pl.BlockSpec(memory_space=pltpu.VMEM)] * 3,
        out_specs=pl.BlockSpec(memory_space=pltpu.VMEM),
        scratch_shapes=[pltpu.VMEM((slots, 128), jnp.int32)],
    )(jnp.transpose(bag_rows, (1, 2, 0)), jnp.transpose(bag_lengths, (1, 0)), counts)
    return message.reshape(groups, pool // 2, 128)


def pool_kernel(
    msg_ref, table_hbm, out_hbm, table_ref, table_f32, pooled, out_ref, ids, ids_smem, sems,
    out_sems, table_sem,
    *, first, rows, pool,
):
    vocab_rows, emb = table_hbm.shape
    table_copy = pltpu.make_async_copy(table_hbm, table_ref, table_sem)
    table_copy.start()
    peers = out_ref.shape[0]
    lanes = ids.shape[1]
    per = min(pool, lanes // rows)
    lines = -(-pool // per)
    shares = sems.shape[0]
    lane = lax.broadcasted_iota(jnp.int32, (peers, lanes), 1)
    held = []
    for h in range(pool // 2):
        word = msg_ref[pl.ds(h, peers, stride=pool // 2), :]
        held += [word & 0xFFFF, lax.shift_right_logical(word, 16)]
    for q in range(lines):
        line = jnp.zeros((peers, lanes), jnp.int32)
        for r in range(per):
            moved = pltpu.roll(held[q * per + r], (r * rows - first) % lanes, 1)
            line = jnp.where((lane >= r * rows) & (lane < (r + 1) * rows), moved, line)
        ids[pl.ds(q, peers, stride=lines), :] = line
    step = peers // shares
    copies = [
        pltpu.make_async_copy(
            ids.at[pl.ds(c * step * lines, step * lines)],
            ids_smem.at[pl.ds(c * step * lines, step * lines)],
            sems.at[c],
        )
        for c in range(shares)
    ]
    for copy in copies:
        copy.start()
    table_f32[pl.ds(vocab_rows, 8), :] = jnp.zeros((8, emb), jnp.float32)
    table_copy.wait()

    def widen(i, carry):
        at = pl.multiple_of(i * 256, 256)
        table_f32[pl.ds(at, 256), :] = table_ref[pl.ds(at, 256), :].astype(jnp.float32)
        return carry

    lax.fori_loop(0, vocab_rows // 256, widen, 0)

    def some_senders(i, carry):
        views = [
            [ids_smem.at[pl.ds((i * SENDERS + n) * lines + q, 1)] for q in range(lines)]
            for n in range(SENDERS)
        ]
        for j in range(rows):
            for n in range(SENDERS):
                parts = [
                    table_f32[pl.ds(views[n][p // per][0, (p % per) * rows + j], 1), :]
                    for p in range(pool)
                ]
                while len(parts) > 1:
                    parts = [parts[m] + parts[m + 1] for m in range(0, len(parts), 2)]
                pooled[pl.ds((i * SENDERS + n) * rows + j, 1), :] = parts[0]
        return carry

    def narrow(d, carry):
        at = pl.multiple_of(d * rows, 8)
        out_ref[d] = pooled[pl.ds(at, rows), :].astype(jnp.bfloat16)
        return carry

    outs = [
        pltpu.make_async_copy(
            out_ref.at[pl.ds(c * step, step)], out_hbm.at[pl.ds(c * step, step)], out_sems.at[c]
        )
        for c in range(shares)
    ]
    for c in range(shares):
        copies[c].wait()
        lax.fori_loop(c * step // SENDERS, (c + 1) * step // SENDERS, some_senders, 0)
        lax.fori_loop(c * step, (c + 1) * step, narrow, 0, unroll=4)
        outs[c].start()
    for c in range(shares):
        outs[c].wait()


def pool_rows(message, table_rows, first, rows):
    peers, halves, width = message.shape
    pool = 2 * halves
    lines = -(-pool // min(pool, width // rows))
    emb = table_rows.shape[1]
    vmem = pl.BlockSpec(memory_space=pltpu.VMEM)
    return pl.pallas_call(
        functools.partial(pool_kernel, first=first, rows=rows, pool=pool),
        out_shape=jax.ShapeDtypeStruct((peers, rows, emb), jnp.bfloat16),
        in_specs=[vmem, pl.BlockSpec(memory_space=pltpu.HBM)],
        out_specs=pl.BlockSpec(memory_space=pltpu.HBM),
        scratch_shapes=[
            pltpu.VMEM(table_rows.shape, jnp.bfloat16),
            pltpu.VMEM((table_rows.shape[0] + 8, emb), jnp.float32),
            pltpu.VMEM((peers * rows, emb), jnp.float32),
            pltpu.VMEM((peers, rows, emb), jnp.bfloat16),
            pltpu.VMEM((peers * lines, width), jnp.int32),
            pltpu.SMEM((peers * lines, width), jnp.int32),
            pltpu.SemaphoreType.DMA((SHARES,)),
            pltpu.SemaphoreType.DMA((SHARES,)),
            pltpu.SemaphoreType.DMA(()),
        ],
        compiler_params=pltpu.CompilerParams(vmem_limit_bytes=125 << 19),
        cost_estimate=pl.CostEstimate(flops=20_000_000_000, bytes_accessed=5 << 20, transcendentals=0),
    )(message.reshape(peers * halves, width), table_rows)


def selector_kernel(pos_ref, out_ref):
    blocks, rows, lanes = out_ref.shape
    pairs = rows // BLOCK
    half = lanes
    lane = lax.broadcasted_iota(jnp.int32, (BLOCK, half), 1).astype(jnp.float32)
    upper = lax.broadcasted_iota(jnp.int32, (BLOCK, pos_ref.shape[1]), 0) < BLOCK // 2

    def one_block(i, carry):
        here = pos_ref[pl.ds(pl.multiple_of(i * BLOCK, BLOCK), BLOCK), :]
        swapped = pltpu.roll(here, BLOCK // 2, 0)
        samples = here.shape[1]
        sides = (
            jnp.where(upper, here, pltpu.roll(swapped, samples - 1, 1)),
            jnp.where(upper, swapped, pltpu.roll(here, samples - 1, 1)),
        )
        for p in range(0, pairs, 2):
            both = []
            for c in (2 * p, 2 * p + 2):
                marks = [
                    jnp.where(jnp.broadcast_to(pos[:, c : c + 1], (BLOCK, half)) == lane, mark, 0.0)
                    for mark, pos in zip((1.0, 2.0), sides)
                ]
                both.append(marks[0] + marks[1])
            out_ref[i, pl.ds(p * BLOCK, 2 * BLOCK), :] = jnp.concatenate(both, axis=0).astype(
                jnp.bfloat16
            )
        return carry

    lax.fori_loop(0, blocks, one_block, 0)


def build_selectors(pos):
    features, samples = pos.shape
    blocks = features // BLOCK
    pairs = samples // 2
    some = 4
    return pl.pallas_call(
        selector_kernel,
        grid=(blocks // some,),
        out_shape=jax.ShapeDtypeStruct((blocks, pairs * BLOCK, 128), jnp.bfloat16),
        in_specs=[pl.BlockSpec((some * BLOCK, samples), lambda i: (i, 0))],
        out_specs=pl.BlockSpec((some, pairs * BLOCK, 128), lambda i: (i, 0, 0)),
        compiler_params=pltpu.CompilerParams(vmem_limit_bytes=8 << 20),
        cost_estimate=pl.CostEstimate(flops=10_000_000_000, bytes_accessed=8 << 20, transcendentals=0),
    )(pos)


def tail_kernel(
    base_ref, selector_ref, compress_ref, weight_ref, bias_ref, arrived_ref, out_ref,
    rows_bf16, rows_f32, feats, pairs, turned, select_vmem, weight_vmem,
    row_sem, select_sem, weight_sem, *, most_rows,
):
    groups, _, emb = arrived_ref.shape
    total_rows = groups * PACK_ROOM
    sample_pairs, _, features, _ = feats.shape
    samples = 2 * sample_pairs
    mixes = compress_ref.shape[0]
    blocks = features // BLOCK
    share = blocks // PARTS
    quarter = groups // 4
    row_copies = [
        pltpu.make_async_copy(
            arrived_ref.at[pl.ds(c * quarter, quarter)],
            rows_bf16.at[pl.ds(c * quarter, quarter)],
            row_sem.at[c],
        )
        for c in range(4)
    ]
    copies = [
        pltpu.make_async_copy(
            selector_ref.at[pl.ds(part * share, share)],
            select_vmem.at[pl.ds(part * share, share)],
            select_sem.at[part],
        )
        for part in range(PARTS)
    ]
    weight_copy = pltpu.make_async_copy(weight_ref, weight_vmem, weight_sem)
    for copy in row_copies + copies[:1]:
        copy.start()

    rows_f32[pl.ds(total_rows, most_rows), :] = jnp.zeros((most_rows, emb), jnp.float32)

    def widen(g, carry):
        at = pl.multiple_of(g * PACK_ROOM, 16)
        rows_f32[pl.ds(at, PACK_ROOM), :] = rows_bf16[g].astype(jnp.float32)
        return carry

    for c in range(4):
        row_copies[c].wait()
        lax.fori_loop(c * quarter, (c + 1) * quarter, widen, 0, unroll=4)
    for copy in copies[1:AHEAD]:
        copy.start()

    first_half = lax.broadcasted_iota(jnp.int32, (1, BLOCK, emb), 1) < BLOCK // 2
    some = 32
    empty = jnp.zeros((BLOCK // 2 * most_rows, emb), jnp.bfloat16)
    zero = jnp.zeros((some * BLOCK, BLOCK // 2 * most_rows), jnp.bfloat16)
    one = jnp.ones_like(zero)
    two = one + one

    def expand(i, carry):
        for pair in range(4):
            tops = []
            for half in range(2):
                block = 8 * i + 2 * pair + half
                sides = []
                for side in range(2):
                    parts = []
                    for j in range(BLOCK // 2):
                        base = base_ref[block * BLOCK + side * (BLOCK // 2) + j]
                        parts.append(rows_f32[pl.ds(base, most_rows), :].astype(jnp.bfloat16))
                    sides.append(jnp.concatenate(parts, axis=0))
                top = jnp.concatenate([sides[0], empty], axis=1)
                bottom = jnp.concatenate([empty, sides[1]], axis=1)
                tops.append((block, jnp.concatenate([top, bottom], axis=0)))
            at = pl.multiple_of((8 * i + 2 * pair) * BLOCK, 2 * BLOCK)
            for c in range(sample_pairs // some):
                even, odd = [], []
                for block, rhs in tops:
                    marks = select_vmem[block, pl.ds(c * some * BLOCK, some * BLOCK), :]
                    second = jnp.where(marks >= two, one, zero)
                    lhs = jnp.concatenate([marks - second - second, second], axis=1)
                    got = jnp.dot(lhs, rhs, preferred_element_type=jnp.float32)
                    got = got.reshape(some, BLOCK, 2 * emb)
                    left, right = got[:, :, :emb], got[:, :, emb:]
                    even.append(jnp.where(first_half, left, pltpu.roll(right, BLOCK // 2, 1)))
                    odd.append(jnp.where(first_half, pltpu.roll(left, BLOCK // 2, 1), right))
                for which, parts in enumerate((even, odd)):
                    feats[pl.ds(c * some, some), which, pl.ds(at, 2 * BLOCK), :] = jnp.concatenate(
                        parts, axis=1
                    ).astype(jnp.bfloat16)
        return carry

    for part in range(PARTS):
        copies[part].wait()
        if part + AHEAD < PARTS:
            copies[part + AHEAD].start()
        if part == WEIGHTS_AT:
            weight_copy.start()
        lax.fori_loop(part * share // 8, (part + 1) * share // 8, expand, 0)

    per = 16

    def score(i, carry):
        mixing = compress_ref[...]
        mixed = []
        for j in range(per // 2):
            at = i * (per // 2) + j
            both = jnp.concatenate([feats[at, 0], feats[at, 1]], axis=1)
            turned[j] = jnp.transpose(both)
            mixed.append(
                jnp.dot(mixing, both, preferred_element_type=jnp.float32).astype(jnp.bfloat16)
            )
        for j in range(per // 2):
            none = jnp.zeros((mixes, emb), jnp.bfloat16)
            first = jnp.concatenate([mixed[j][:, :emb], none], axis=1)
            second = jnp.concatenate([none, mixed[j][:, emb:]], axis=1)
            lhs = jnp.concatenate([first, second], axis=0)
            got = jnp.dot(lhs, turned[j], preferred_element_type=jnp.float32)
            for n in range(2 * mixes // BLOCK):
                sample = i * per + 2 * j + n * BLOCK // mixes
                at = pl.multiple_of(sample * BLOCK, BLOCK)
                for c in range(features // 128):
                    pairs[c, n % (mixes // BLOCK), pl.ds(at, BLOCK), :] = got[
                        n * BLOCK : (n + 1) * BLOCK, c * 128 : (c + 1) * 128
                    ]
        return carry

    lax.fori_loop(0, samples // per, score, 0)

    weight_copy.wait()
    total = jnp.broadcast_to(bias_ref[...], (samples, out_ref.shape[1]))
    for k in range(mixes):
        lhs = jnp.concatenate(
            [
                pairs[c, k // BLOCK, pl.ds(k % BLOCK, samples, stride=BLOCK), :]
                for c in range(features // 128)
            ],
            axis=1,
        ).astype(jnp.bfloat16)
        total = total + jnp.dot(lhs, weight_vmem[k], preferred_element_type=jnp.float32)
    out_ref[...] = jnp.maximum(total, 0.0).astype(jnp.bfloat16)


def score_samples(base, selectors, arrived, compress, weight, bias, most_rows):
    mixes, features = compress.shape
    units = weight.shape[2]
    groups, _, emb = arrived.shape
    samples = 2 * selectors.shape[1] // BLOCK
    vmem = pl.BlockSpec(memory_space=pltpu.VMEM)
    hbm = pl.BlockSpec(memory_space=pltpu.HBM)
    return pl.pallas_call(
        functools.partial(tail_kernel, most_rows=most_rows),
        out_shape=jax.ShapeDtypeStruct((samples, units), jnp.bfloat16),
        in_specs=[pl.BlockSpec(memory_space=pltpu.SMEM), hbm, vmem, hbm, vmem, hbm],
        out_specs=vmem,
        scratch_shapes=[
            pltpu.VMEM(arrived.shape, jnp.bfloat16),
            pltpu.VMEM((groups * PACK_ROOM + most_rows, emb), jnp.float32),
            pltpu.VMEM((samples // 2, 2, features, emb), jnp.bfloat16),
            pltpu.VMEM((features // 128, mixes // BLOCK, samples * BLOCK, 128), jnp.float32),
            pltpu.VMEM((8, 2 * emb, features), jnp.bfloat16),
            pltpu.VMEM(selectors.shape, jnp.bfloat16),
            pltpu.VMEM(weight.shape, jnp.bfloat16),
            pltpu.SemaphoreType.DMA((4,)),
            pltpu.SemaphoreType.DMA((PARTS,)),
            pltpu.SemaphoreType.DMA(()),
        ],
        compiler_params=pltpu.CompilerParams(vmem_limit_bytes=125 << 19),
        cost_estimate=pl.CostEstimate(flops=20_000_000_000, bytes_accessed=16 << 20, transcendentals=0),
    )(base, selectors, compress, weight, bias, arrived)


def shards(
    tables, bag_rows, bag_lengths, row_counts, inverse, table_order, compress, top_weight, top_bias
):
    vocabulary, emb = tables.shape[1:]
    slots = table_order.shape[0]
    most_rows = bag_rows.shape[2]
    mixes = compress.shape[0]
    counts = row_counts[0]
    message = bag_message(bag_rows[0], bag_lengths[0], row_counts, vocabulary)
    got = lax.all_to_all(message, "dev", split_axis=0, concat_axis=0, tiled=True)
    table_rows = tables.reshape(-1, emb)
    pooled = pool_rows(got, table_rows, 0, PACK_ROOM)
    arrived = lax.all_to_all(pooled, "dev", split_axis=0, concat_axis=0, tiled=True)

    grouped = counts.reshape(-1, GROUP)
    before = jnp.cumsum(grouped, axis=1) - grouped
    group_at = jnp.arange(slots // GROUP, dtype=jnp.int32)[:, None] * PACK_ROOM
    slot_base = (before + group_at).reshape(-1)
    slot_range = jnp.arange(slots, dtype=jnp.int32)
    matches = table_order[:, None] == slot_range[None, :]
    feature_base = jnp.sum(jnp.where(matches, slot_base[:, None], 0), axis=0)
    feature_count = jnp.sum(jnp.where(matches, counts[:, None], 0), axis=0)
    shift = (slot_range % (BLOCK // 2)) * most_rows
    pos = jnp.where(inverse < feature_count[None, :], inverse + shift[None, :], -1)
    selectors = build_selectors(jnp.transpose(pos.astype(jnp.float32), (1, 0)))
    weight = jnp.transpose(top_weight.reshape(slots, mixes, -1), (1, 0, 2))
    return score_samples(
        feature_base, selectors, arrived, compress, weight, top_bias[None, :], most_rows
    )


def solution(mesh):
    return jax.shard_map(
        shards,
        mesh=mesh,
        in_specs=(
            P("dev", None, None),
            P(("rep", "dev"), None, None, None),
            P(("rep", "dev"), None, None),
            P(("rep", "dev"), None),
            P(("rep", "dev"), None),
            P(),
            P(),
            P(),
            P(),
        ),
        out_specs=P(("rep", "dev"), None),
        check_vma=False,
    )
```

```python
import functools

import jax
import jax.numpy as jnp
from jax import lax
from jax.experimental import pallas as pl
from jax.experimental.pallas import tpu as pltpu
from jax.sharding import PartitionSpec as P

PACK_ROOM = 80
BLOCK = 8
PARTS = 8
AHEAD = 3
WEIGHTS_AT = 5
SENDERS = 2
SHARES = 4
GROUP = 4


def message_kernel(ids_ref, lengths_ref, counts_ref, out_ref, words, *, vocabulary):
    most_rows, pool, slots = ids_ref.shape
    spare = GROUP * vocabulary
    slot = lax.broadcasted_iota(jnp.int32, (8, slots), 1) % GROUP
    counts = jnp.broadcast_to(counts_ref[...], (8, slots))
    offset = jnp.zeros((8, slots), jnp.int32)
    for back in range(1, GROUP):
        offset = offset + jnp.where(slot >= back, pltpu.roll(counts, back, 1), 0)
    offset = offset[:1, :]
    table = slot[:1, :] * vocabulary
    lengths = lengths_ref[...]
    used = lax.broadcasted_iota(jnp.int32, (most_rows, slots), 0) < counts[:1, :]
    room = 128
    for h in range(pool // 2):
        low = jnp.where(2 * h < lengths, ids_ref[:, 2 * h, :] + table, spare)
        high = jnp.where(2 * h + 1 < lengths, ids_ref[:, 2 * h + 1, :] + table, spare)
        word = jnp.where(used, low | (high << 16), 0)
        word = jnp.concatenate([word, jnp.zeros((8, slots), jnp.int32)], axis=0)
        for bit in range(3):
            moved = pltpu.roll(word, 1 << bit, 0)
            word = jnp.where(((offset >> bit) & 1) == 1, moved, word)
        word = jnp.concatenate(
            [word, jnp.zeros((room - word.shape[0], slots), jnp.int32)], axis=0
        )
        for bit in range(3, 7):
            by = 1 << bit
            moved = jnp.concatenate(
                [jnp.zeros((by, slots), jnp.int32), word[: room - by, :]], axis=0
            )
            word = jnp.where(((offset >> bit) & 1) == 1, moved, word)
        words[...] = jnp.transpose(word, (1, 0))
        groups = slots // GROUP
        total = words[pl.ds(0, groups, stride=GROUP), :]
        for member in range(1, GROUP):
            total = total + words[pl.ds(member, groups, stride=GROUP), :]
        out_ref[pl.ds(h, groups, stride=pool // 2), :] = total


def bag_message(bag_rows, bag_lengths, counts, vocabulary):
    slots, most_rows, pool = bag_rows.shape
    groups = slots // GROUP
    message = pl.pallas_call(
        functools.partial(message_kernel, vocabulary=vocabulary),
        out_shape=jax.ShapeDtypeStruct((groups * pool // 2, 128), jnp.int32),
        in_specs=[pl.BlockSpec(memory_space=pltpu.VMEM)] * 3,
        out_specs=pl.BlockSpec(memory_space=pltpu.VMEM),
        scratch_shapes=[pltpu.VMEM((slots, 128), jnp.int32)],
    )(jnp.transpose(bag_rows, (1, 2, 0)), jnp.transpose(bag_lengths, (1, 0)), counts)
    return message.reshape(groups, pool // 2, 128)


def pool_kernel(
    msg_ref, table_hbm, out_hbm, table_ref, table_f32, pooled, out_ref, ids, ids_smem, sems,
    out_sems, table_sem,
    *, first, rows, pool,
):
    vocab_rows, emb = table_hbm.shape
    table_copy = pltpu.make_async_copy(table_hbm, table_ref, table_sem)
    table_copy.start()
    peers = out_ref.shape[0]
    lanes = ids.shape[1]
    per = min(pool, lanes // rows)
    lines = -(-pool // per)
    shares = sems.shape[0]
    lane = lax.broadcasted_iota(jnp.int32, (peers, lanes), 1)
    held = []
    for h in range(pool // 2):
        word = msg_ref[pl.ds(h, peers, stride=pool // 2), :]
        held += [word & 0xFFFF, lax.shift_right_logical(word, 16)]
    for q in range(lines):
        line = jnp.zeros((peers, lanes), jnp.int32)
        for r in range(per):
            moved = pltpu.roll(held[q * per + r], (r * rows - first) % lanes, 1)
            line = jnp.where((lane >= r * rows) & (lane < (r + 1) * rows), moved, line)
        ids[pl.ds(q, peers, stride=lines), :] = line
    step = peers // shares
    copies = [
        pltpu.make_async_copy(
            ids.at[pl.ds(c * step * lines, step * lines)],
            ids_smem.at[pl.ds(c * step * lines, step * lines)],
            sems.at[c],
        )
        for c in range(shares)
    ]
    for copy in copies:
        copy.start()
    table_f32[pl.ds(vocab_rows, 8), :] = jnp.zeros((8, emb), jnp.float32)
    table_copy.wait()

    def widen(i, carry):
        at = pl.multiple_of(i * 256, 256)
        table_f32[pl.ds(at, 256), :] = table_ref[pl.ds(at, 256), :].astype(jnp.float32)
        return carry

    lax.fori_loop(0, vocab_rows // 256, widen, 0)

    def some_senders(i, carry):
        views = [
            [ids_smem.at[pl.ds((i * SENDERS + n) * lines + q, 1)] for q in range(lines)]
            for n in range(SENDERS)
        ]
        for j in range(rows):
            for n in range(SENDERS):
                parts = [
                    table_f32[pl.ds(views[n][p // per][0, (p % per) * rows + j], 1), :]
                    for p in range(pool)
                ]
                while len(parts) > 1:
                    parts = [parts[m] + parts[m + 1] for m in range(0, len(parts), 2)]
                pooled[pl.ds((i * SENDERS + n) * rows + j, 1), :] = parts[0]
        return carry

    def narrow(d, carry):
        at = pl.multiple_of(d * rows, 8)
        out_ref[d] = pooled[pl.ds(at, rows), :].astype(jnp.bfloat16)
        return carry

    outs = [
        pltpu.make_async_copy(
            out_ref.at[pl.ds(c * step, step)], out_hbm.at[pl.ds(c * step, step)], out_sems.at[c]
        )
        for c in range(shares)
    ]
    for c in range(shares):
        copies[c].wait()
        lax.fori_loop(c * step // SENDERS, (c + 1) * step // SENDERS, some_senders, 0)
        lax.fori_loop(c * step, (c + 1) * step, narrow, 0, unroll=4)
        outs[c].start()
    for c in range(shares):
        outs[c].wait()


def pool_rows(message, table_rows, first, rows):
    peers, halves, width = message.shape
    pool = 2 * halves
    lines = -(-pool // min(pool, width // rows))
    emb = table_rows.shape[1]
    vmem = pl.BlockSpec(memory_space=pltpu.VMEM)
    return pl.pallas_call(
        functools.partial(pool_kernel, first=first, rows=rows, pool=pool),
        out_shape=jax.ShapeDtypeStruct((peers, rows, emb), jnp.bfloat16),
        in_specs=[vmem, pl.BlockSpec(memory_space=pltpu.HBM)],
        out_specs=pl.BlockSpec(memory_space=pltpu.HBM),
        scratch_shapes=[
            pltpu.VMEM(table_rows.shape, jnp.bfloat16),
            pltpu.VMEM((table_rows.shape[0] + 8, emb), jnp.float32),
            pltpu.VMEM((peers * rows, emb), jnp.float32),
            pltpu.VMEM((peers, rows, emb), jnp.bfloat16),
            pltpu.VMEM((peers * lines, width), jnp.int32),
            pltpu.SMEM((peers * lines, width), jnp.int32),
            pltpu.SemaphoreType.DMA((SHARES,)),
            pltpu.SemaphoreType.DMA((SHARES,)),
            pltpu.SemaphoreType.DMA(()),
        ],
        compiler_params=pltpu.CompilerParams(vmem_limit_bytes=125 << 19),
        cost_estimate=pl.CostEstimate(flops=20_000_000_000, bytes_accessed=5 << 20, transcendentals=0),
    )(message.reshape(peers * halves, width), table_rows)


def selector_kernel(pos_ref, out_ref):
    blocks, rows, lanes = out_ref.shape
    pairs = rows // BLOCK
    half = lanes
    lane = lax.broadcasted_iota(jnp.int32, (BLOCK, half), 1).astype(jnp.float32)
    upper = lax.broadcasted_iota(jnp.int32, (BLOCK, pos_ref.shape[1]), 0) < BLOCK // 2

    def one_block(i, carry):
        here = pos_ref[pl.ds(pl.multiple_of(i * BLOCK, BLOCK), BLOCK), :]
        swapped = pltpu.roll(here, BLOCK // 2, 0)
        samples = here.shape[1]
        sides = (
            jnp.where(upper, here, pltpu.roll(swapped, samples - 1, 1)),
            jnp.where(upper, swapped, pltpu.roll(here, samples - 1, 1)),
        )
        for p in range(0, pairs, 2):
            both = []
            for c in (2 * p, 2 * p + 2):
                marks = [
                    jnp.where(jnp.broadcast_to(pos[:, c : c + 1], (BLOCK, half)) == lane, mark, 0.0)
                    for mark, pos in zip((1.0, 2.0), sides)
                ]
                both.append(marks[0] + marks[1])
            out_ref[i, pl.ds(p * BLOCK, 2 * BLOCK), :] = jnp.concatenate(both, axis=0).astype(
                jnp.bfloat16
            )
        return carry

    lax.fori_loop(0, blocks, one_block, 0)


def build_selectors(pos):
    features, samples = pos.shape
    blocks = features // BLOCK
    pairs = samples // 2
    some = 4
    return pl.pallas_call(
        selector_kernel,
        grid=(blocks // some,),
        out_shape=jax.ShapeDtypeStruct((blocks, pairs * BLOCK, 128), jnp.bfloat16),
        in_specs=[pl.BlockSpec((some * BLOCK, samples), lambda i: (i, 0))],
        out_specs=pl.BlockSpec((some, pairs * BLOCK, 128), lambda i: (i, 0, 0)),
        compiler_params=pltpu.CompilerParams(vmem_limit_bytes=8 << 20),
        cost_estimate=pl.CostEstimate(flops=10_000_000_000, bytes_accessed=8 << 20, transcendentals=0),
    )(pos)


def tail_kernel(
    base_ref, selector_ref, compress_ref, weight_ref, bias_ref, arrived_ref, out_ref,
    rows_bf16, rows_f32, feats, pairs, turned, select_vmem, weight_vmem,
    row_sem, select_sem, weight_sem, *, most_rows,
):
    groups, _, emb = arrived_ref.shape
    total_rows = groups * PACK_ROOM
    sample_pairs, _, features, _ = feats.shape
    samples = 2 * sample_pairs
    mixes = compress_ref.shape[0]
    blocks = features // BLOCK
    share = blocks // PARTS
    quarter = groups // 4
    row_copies = [
        pltpu.make_async_copy(
            arrived_ref.at[pl.ds(c * quarter, quarter)],
            rows_bf16.at[pl.ds(c * quarter, quarter)],
            row_sem.at[c],
        )
        for c in range(4)
    ]
    copies = [
        pltpu.make_async_copy(
            selector_ref.at[pl.ds(part * share, share)],
            select_vmem.at[pl.ds(part * share, share)],
            select_sem.at[part],
        )
        for part in range(PARTS)
    ]
    weight_copy = pltpu.make_async_copy(weight_ref, weight_vmem, weight_sem)
    for copy in row_copies + copies[:1]:
        copy.start()

    rows_f32[pl.ds(total_rows, most_rows), :] = jnp.zeros((most_rows, emb), jnp.float32)

    def widen(g, carry):
        at = pl.multiple_of(g * PACK_ROOM, 16)
        rows_f32[pl.ds(at, PACK_ROOM), :] = rows_bf16[g].astype(jnp.float32)
        return carry

    for c in range(4):
        row_copies[c].wait()
        lax.fori_loop(c * quarter, (c + 1) * quarter, widen, 0, unroll=4)
    for copy in copies[1:AHEAD]:
        copy.start()

    first_half = lax.broadcasted_iota(jnp.int32, (1, BLOCK, emb), 1) < BLOCK // 2
    some = 32
    empty = jnp.zeros((BLOCK // 2 * most_rows, emb), jnp.bfloat16)
    zero = jnp.zeros((some * BLOCK, BLOCK // 2 * most_rows), jnp.bfloat16)
    one = jnp.ones_like(zero)
    two = one + one

    def expand(i, carry):
        for pair in range(4):
            tops = []
            for half in range(2):
                block = 8 * i + 2 * pair + half
                sides = []
                for side in range(2):
                    parts = []
                    for j in range(BLOCK // 2):
                        base = base_ref[block * BLOCK + side * (BLOCK // 2) + j]
                        parts.append(rows_f32[pl.ds(base, most_rows), :].astype(jnp.bfloat16))
                    sides.append(jnp.concatenate(parts, axis=0))
                top = jnp.concatenate([sides[0], empty], axis=1)
                bottom = jnp.concatenate([empty, sides[1]], axis=1)
                tops.append((block, jnp.concatenate([top, bottom], axis=0)))
            at = pl.multiple_of((8 * i + 2 * pair) * BLOCK, 2 * BLOCK)
            for c in range(sample_pairs // some):
                even, odd = [], []
                for block, rhs in tops:
                    marks = select_vmem[block, pl.ds(c * some * BLOCK, some * BLOCK), :]
                    second = jnp.where(marks >= two, one, zero)
                    lhs = jnp.concatenate([marks - second - second, second], axis=1)
                    got = jnp.dot(lhs, rhs, preferred_element_type=jnp.float32)
                    got = got.reshape(some, BLOCK, 2 * emb)
                    left, right = got[:, :, :emb], got[:, :, emb:]
                    even.append(jnp.where(first_half, left, pltpu.roll(right, BLOCK // 2, 1)))
                    odd.append(jnp.where(first_half, pltpu.roll(left, BLOCK // 2, 1), right))
                for which, parts in enumerate((even, odd)):
                    feats[pl.ds(c * some, some), which, pl.ds(at, 2 * BLOCK), :] = jnp.concatenate(
                        parts, axis=1
                    ).astype(jnp.bfloat16)
        return carry

    for part in range(PARTS):
        copies[part].wait()
        if part + AHEAD < PARTS:
            copies[part + AHEAD].start()
        if part == WEIGHTS_AT:
            weight_copy.start()
        lax.fori_loop(part * share // 8, (part + 1) * share // 8, expand, 0)

    per = 32

    def score(i, carry):
        mixing = compress_ref[...]
        mixed = []
        for j in range(per // 2):
            at = i * (per // 2) + j
            both = jnp.concatenate([feats[at, 0], feats[at, 1]], axis=1)
            turned[j] = jnp.transpose(both)
            mixed.append(
                jnp.dot(mixing, both, preferred_element_type=jnp.float32).astype(jnp.bfloat16)
            )
        for j in range(per // 2):
            none = jnp.zeros((mixes, emb), jnp.bfloat16)
            first = jnp.concatenate([mixed[j][:, :emb], none], axis=1)
            second = jnp.concatenate([none, mixed[j][:, emb:]], axis=1)
            lhs = jnp.concatenate([first, second], axis=0)
            got = jnp.dot(lhs, turned[j], preferred_element_type=jnp.float32)
            for n in range(2 * mixes // BLOCK):
                sample = i * per + 2 * j + n * BLOCK // mixes
                at = pl.multiple_of(sample * BLOCK, BLOCK)
                for c in range(features // 128):
                    pairs[c, n % (mixes // BLOCK), pl.ds(at, BLOCK), :] = got[
                        n * BLOCK : (n + 1) * BLOCK, c * 128 : (c + 1) * 128
                    ]
        return carry

    lax.fori_loop(0, samples // per, score, 0)

    weight_copy.wait()
    total = jnp.broadcast_to(bias_ref[...], (samples, out_ref.shape[1]))
    for k in range(mixes):
        lhs = jnp.concatenate(
            [
                pairs[c, k // BLOCK, pl.ds(k % BLOCK, samples, stride=BLOCK), :]
                for c in range(features // 128)
            ],
            axis=1,
        ).astype(jnp.bfloat16)
        total = total + jnp.dot(lhs, weight_vmem[k], preferred_element_type=jnp.float32)
    out_ref[...] = jnp.maximum(total, 0.0).astype(jnp.bfloat16)


def score_samples(base, selectors, arrived, compress, weight, bias, most_rows):
    mixes, features = compress.shape
    units = weight.shape[2]
    groups, _, emb = arrived.shape
    samples = 2 * selectors.shape[1] // BLOCK
    vmem = pl.BlockSpec(memory_space=pltpu.VMEM)
    hbm = pl.BlockSpec(memory_space=pltpu.HBM)
    return pl.pallas_call(
        functools.partial(tail_kernel, most_rows=most_rows),
        out_shape=jax.ShapeDtypeStruct((samples, units), jnp.bfloat16),
        in_specs=[pl.BlockSpec(memory_space=pltpu.SMEM), hbm, vmem, hbm, vmem, hbm],
        out_specs=vmem,
        scratch_shapes=[
            pltpu.VMEM(arrived.shape, jnp.bfloat16),
            pltpu.VMEM((groups * PACK_ROOM + most_rows, emb), jnp.float32),
            pltpu.VMEM((samples // 2, 2, features, emb), jnp.bfloat16),
            pltpu.VMEM((features // 128, mixes // BLOCK, samples * BLOCK, 128), jnp.float32),
            pltpu.VMEM((16, 2 * emb, features), jnp.bfloat16),
            pltpu.VMEM(selectors.shape, jnp.bfloat16),
            pltpu.VMEM(weight.shape, jnp.bfloat16),
            pltpu.SemaphoreType.DMA((4,)),
            pltpu.SemaphoreType.DMA((PARTS,)),
            pltpu.SemaphoreType.DMA(()),
        ],
        compiler_params=pltpu.CompilerParams(vmem_limit_bytes=125 << 19),
        cost_estimate=pl.CostEstimate(flops=20_000_000_000, bytes_accessed=16 << 20, transcendentals=0),
    )(base, selectors, compress, weight, bias, arrived)


def shards(
    tables, bag_rows, bag_lengths, row_counts, inverse, table_order, compress, top_weight, top_bias
):
    vocabulary, emb = tables.shape[1:]
    slots = table_order.shape[0]
    most_rows = bag_rows.shape[2]
    mixes = compress.shape[0]
    counts = row_counts[0]
    message = bag_message(bag_rows[0], bag_lengths[0], row_counts, vocabulary)
    got = lax.all_to_all(message, "dev", split_axis=0, concat_axis=0, tiled=True)
    table_rows = tables.reshape(-1, emb)
    pooled = pool_rows(got, table_rows, 0, PACK_ROOM)
    arrived = lax.all_to_all(pooled, "dev", split_axis=0, concat_axis=0, tiled=True)

    grouped = counts.reshape(-1, GROUP)
    before = jnp.cumsum(grouped, axis=1) - grouped
    group_at = jnp.arange(slots // GROUP, dtype=jnp.int32)[:, None] * PACK_ROOM
    slot_base = (before + group_at).reshape(-1)
    slot_range = jnp.arange(slots, dtype=jnp.int32)
    matches = table_order[:, None] == slot_range[None, :]
    feature_base = jnp.sum(jnp.where(matches, slot_base[:, None], 0), axis=0)
    feature_count = jnp.sum(jnp.where(matches, counts[:, None], 0), axis=0)
    shift = (slot_range % (BLOCK // 2)) * most_rows
    pos = jnp.where(inverse < feature_count[None, :], inverse + shift[None, :], -1)
    selectors = build_selectors(jnp.transpose(pos.astype(jnp.float32), (1, 0)))
    weight = jnp.transpose(top_weight.reshape(slots, mixes, -1), (1, 0, 2))
    return score_samples(
        feature_base, selectors, arrived, compress, weight, top_bias[None, :], most_rows
    )


def solution(mesh):
    return jax.shard_map(
        shards,
        mesh=mesh,
        in_specs=(
            P("dev", None, None),
            P(("rep", "dev"), None, None, None),
            P(("rep", "dev"), None, None),
            P(("rep", "dev"), None),
            P(("rep", "dev"), None),
            P(),
            P(),
            P(),
            P(),
        ),
        out_specs=P(("rep", "dev"), None),
        check_vma=False,
    )
```
